32 devices in a mesh: row: 16 (over z, y, x), col: 2 (over core).
Axes of the slice: x: 2, y: 2, z: 4, core: 2. Of those that a mesh axis runs over, the one named last changes fastest.
Arguments:
- sources: bfloat16 [32768, 640], P(('row', 'col')), may hold values from -6 to 6
- tree_perm: int32 [32768], P(('row', 'col')), may hold values from 0 to 32767, as said below
- leaf_blocks: bfloat16 [32768, 512], P(('row', 'col')), may hold values from -0.25 to 0.25
- u_factors: bfloat16 [6, 32, 32768], P(None, None, ('row', 'col')), may hold values from -0.4375 to 0.4375
- v_factors: bfloat16 [6, 32, 32768], P(None, None, ('row', 'col')), as said below
- level_ranks: int32 [6], replicated, may hold values from 16 to 32
Outputs:
- products: bfloat16 [32768, 640], P(('row', 'col'))
The draws below stay inside these ranges and needn't reach their ends.
Inputs may be any that keep to these rules, and one draw needn't show every extreme that they name: tree_perm is a permutation that maps each aligned block of 1024 positions onto the same block of initial indices. `v_factors`: entries of level l are of the order of the inverse square root of 32768 / 2^l.
All inputs are finite; a program needn't handle non-finite values.
Results may differ from the reference program's by a relative error of at most 0.0037.
Values sent between devices are 32-bit elements; how exact they have to be, the bound alone decides.
No kernel may reach another device: no remote copies, remote signals or barrier semaphores. Data moves between devices by JAX's collectives and lax.ppermute only.
A program may use at most 64 MiB of HBM per device.

```python
import jax
import jax.numpy as jnp
from jax import lax

LEAF = 512
K = 32
RHS = 640
ROWS_DEV = 1024
N = 32768
LEVELS = 6


def draw_tree_perm(key, part):
    blocks = N // ROWS_DEV
    keys = jax.random.split(key, blocks)
    perms = jax.vmap(lambda one_key: jax.random.permutation(one_key, ROWS_DEV))(keys).astype(jnp.int32)
    offsets = jnp.arange(blocks, dtype=jnp.int32)[:, None] * ROWS_DEV
    return (perms + offsets).reshape(N).astype(jnp.int32)


def draw_v_factors(key, part):
    level_scale = jnp.sqrt(2.0 ** (jnp.arange(LEVELS, dtype=jnp.float32) + 1.0) / N)
    base = jax.random.normal(key, (LEVELS, K, N), jnp.float32)
    return (base * level_scale[:, None, None]).astype(jnp.bfloat16)


def set_ends(array, stream_key, low, top_value):
    shape = array.shape
    place = [jax.random.randint(jax.random.fold_in(stream_key, axis), (), 0, shape[axis]) for axis in range(len(shape))]
    array = array.at[tuple(place)].set(low)
    longest = shape.index(max(shape))
    place[longest] = (place[longest] + 1) % shape[longest]
    return array.at[tuple(place)].set(top_value)


def levels(rng, extent, cuts, smallest, largest):
    level = 1.0
    for dim, blocks in cuts:
        steps = jax.random.uniform(jax.random.fold_in(jax.random.fold_in(rng, 6), dim), (blocks,), jnp.float32, smallest / len(cuts), largest / len(cuts))
        level = level * jnp.repeat(jnp.exp(steps), extent[dim] // blocks).reshape((-1,) + (1,) * (len(extent) - 1 - dim))
    return level


def bell_draw(stream_key, shape, width, most, cuts=(), held_as=jnp.bfloat16):
    array = width * jax.random.normal(stream_key, shape, jnp.float32)
    if cuts:
        array = array * levels(stream_key, shape, cuts, -0.22, 0.18)
    return jnp.clip(array, -most, most).astype(held_as)


def setup_inputs(seed: int = 0) -> dict:
    arg_keys = jax.random.split(jax.random.key(seed), 7)
    return {
        "sources": bell_draw(arg_keys[0], (N, RHS), 1.0, 6.0, ((0, 32),)),
        "tree_perm": draw_tree_perm(jax.random.fold_in(arg_keys[6], 71), 0),
        "leaf_blocks": bell_draw(arg_keys[2], (N, LEAF), LEAF ** -0.5, 0.25, ((0, 32),)),
        "u_factors": bell_draw(arg_keys[3], (LEVELS, K, N), (K * LEVELS) ** -0.5, 0.4375, ((2, 32),)),
        "v_factors": draw_v_factors(jax.random.fold_in(arg_keys[6], 71), 0),
        "level_ranks": set_ends(jax.random.randint(arg_keys[5], (LEVELS,), K // 2, K + 1), jax.random.fold_in(arg_keys[5], 1), K // 2, K).astype(jnp.int32),
    }


def reference(sources, tree_perm, leaf_blocks, u_factors, v_factors, level_ranks):
    ordered = sources[tree_perm].astype(jnp.float32)
    leaf_count = N // LEAF
    result = jnp.einsum("gij,gjr->gir", leaf_blocks.reshape(leaf_count, LEAF, LEAF).astype(jnp.float32), ordered.reshape(leaf_count, LEAF, RHS)).reshape(N, RHS)
    rank_index = lax.iota(jnp.int32, K)
    for level in range(LEVELS):
        groups = 2 ** (level + 1)
        cluster_rows = N // groups
        v_level = v_factors[level].astype(jnp.float32).reshape(K, groups, cluster_rows)
        coef = jnp.einsum("kgs,gsr->gkr", v_level, ordered.reshape(groups, cluster_rows, RHS))
        far_coef = coef.reshape(groups // 2, 2, K, RHS)[:, ::-1].reshape(groups, K, RHS)
        rank_mask = (rank_index < level_ranks[level]).astype(jnp.float32)
        far_coef = (far_coef * rank_mask[None, :, None]).astype(jnp.bfloat16).astype(jnp.float32)
        u_level = u_factors[level].astype(jnp.float32).reshape(K, groups, cluster_rows)
        result = result + jnp.einsum("kgs,gkr->gsr", u_level, far_coef).reshape(N, RHS)
    tree_out = result.astype(jnp.bfloat16)
    return jnp.zeros((N, RHS), jnp.bfloat16).at[tree_perm].set(tree_out)
```

```python
import functools

import jax
import jax.numpy as jnp
from jax import lax
from jax.experimental import pallas as pl
from jax.experimental.pallas import tpu as pltpu
from jax.sharding import PartitionSpec as P

AXES = ("row", "col")
BF16, F32 = jnp.bfloat16, jnp.float32


def partner(x, bit):
    count = lax.axis_size("row") * lax.axis_size("col")
    return lax.ppermute(x, AXES, [(i, i ^ 1 << bit) for i in range(count)])


def local_positions(perm_ref, row_count):
    return lax.rem(perm_ref[...], row_count)


def fill_select(select_ref, index):
    blocks, width = index.shape
    columns = index.T
    lane = lax.broadcasted_iota(jnp.int32, (width, blocks * width), 1)
    for block in range(blocks):
        hit = lane == columns[:, block : block + 1]
        select_ref[block * width : (block + 1) * width, :] = jnp.where(hit, 1.0, 0.0).astype(BF16)


def fill_select_t(select_ref, index):
    blocks, width = index.shape
    sublane = lax.broadcasted_iota(jnp.int32, (blocks * width, width), 0)
    for block in range(blocks):
        hit = sublane == index[block : block + 1, :]
        select_ref[:, block * width : (block + 1) * width] = jnp.where(hit, 1.0, 0.0).astype(BF16)


def dot(a, b):
    return jnp.dot(a, b, preferred_element_type=F32)


def dot_t(a, b):
    return lax.dot_general(a, b, (((1,), (1,)), ((), ())), preferred_element_type=F32)


def coef_kernel(dev_bits, ranks_ref, perm_ref, v_ref, sources_ref, send_ref, keep_ref,
                select, v_rows, sources, sem):
    copy = pltpu.make_async_copy(sources_ref, sources, sem)
    copy.start()
    rank_cap, row_count = v_ref.shape[1:]
    half = rank_cap // 2
    coarse = (dev_bits - 1) * half
    core = lax.rem(lax.axis_index("col"), 2)
    fill_select(select, local_positions(perm_ref, row_count))
    iota = lax.broadcasted_iota(jnp.int32, (half, 1), 0)

    def masked(level, start):
        rows = v_ref[level, pl.ds(pl.multiple_of(start, half), half), :]
        keep = iota + start < ranks_ref[level]
        return jnp.where(keep, rows.astype(F32), 0.0).astype(BF16)

    for level in range(dev_bits - 1):
        v_rows[level * half : (level + 1) * half, :] = masked(level, (1 - core) * half)
        at = coarse + rank_cap + level * half
        v_rows[at : at + half, :] = masked(level, core * half)
    for part in range(2):
        at = coarse + part * half
        v_rows[at : at + half, :] = masked(dev_bits - 1, jnp.int32(part * half))
    v_local = dot(v_rows[...], select[...]).astype(BF16)
    copy.wait()
    coef = dot(v_local, sources[...])
    send_ref[...] = coef[: coarse + rank_cap]
    keep_ref[...] = coef[coarse + rank_cap :]


def order_kernel(perm_ref, sources_ref, ordered_ref, select):
    row_count = sources_ref.shape[0]
    fill_select(select, local_positions(perm_ref, row_count))
    ordered_ref[...] = dot(select[...], sources_ref[...]).astype(BF16)


def near_kernel(dev_bits, ranks_ref, perm_ref, leaf_ref, u_ref, v_ref, ordered_ref,
                near_ref, u_far_ref, select_t, left, right):
    level_count, rank_cap, row_count = u_ref.shape
    half = rank_cap // 2
    leaf_size = leaf_ref.shape[1]
    core = lax.rem(lax.axis_index("col"), 2)
    fill_select_t(select_t, local_positions(perm_ref, row_count))
    for leaf in range(row_count // leaf_size):
        at = slice(leaf * leaf_size, (leaf + 1) * leaf_size)
        left[:, at] = dot(select_t[:, at], leaf_ref[at, :]).astype(BF16)
    right[:row_count, :] = ordered_ref[...]
    column = row_count
    iota = lax.broadcasted_iota(jnp.int32, (rank_cap, 1), 0)
    for level in range(dev_bits, level_count):
        cluster = row_count >> level - dev_bits + 1
        keep = iota < ranks_ref[level]
        for group in range(row_count // cluster):
            at = slice(group * cluster, (group + 1) * cluster)
            coef = dot(v_ref[level, :, at], ordered_ref[at, :])
            other = column + (group ^ 1) * rank_cap
            right[other : other + rank_cap, :] = jnp.where(keep, coef, 0.0).astype(BF16)
            mine = column + group * rank_cap
            left[:, mine : mine + rank_cap] = dot_t(select_t[:, at], u_ref[level, :, at]).astype(BF16)
        column += row_count // cluster * rank_cap
    near_ref[...] = dot(left[...], right[...])
    coarse = (dev_bits - 1) * half
    rows = []
    for start in (core * half, (1 - core) * half):
        for level in range(dev_bits - 1):
            rows.append(u_ref[level, pl.ds(pl.multiple_of(start, half), half), :])
    rows.append(u_ref[dev_bits - 1])
    u_rows = jnp.concatenate(rows, axis=0)
    u_far_ref[...] = dot_t(select_t[...], u_rows).astype(BF16)


def far_kernel(block, near_ref, u_far_ref, mine_ref, other_ref, sibling_ref, out_ref, far, out, sems):
    coarse, rank_cap = mine_ref.shape[0], sibling_ref.shape[0]
    far[:coarse, :] = mine_ref[...].astype(BF16)
    far[coarse : 2 * coarse, :] = other_ref[...].astype(BF16)
    far[2 * coarse :, :] = sibling_ref[...].astype(BF16)
    copies = []
    for step in range(near_ref.shape[0] // block):
        at = slice(step * block, (step + 1) * block)
        out[at, :] = (near_ref[at, :] + dot(u_far_ref[at, :], far[...])).astype(BF16)
        copy = pltpu.make_async_copy(out.at[at, :], out_ref.at[at, :], sems.at[step])
        copy.start()
        copies.append(copy)
    for copy in copies:
        copy.wait()


VMEM = pl.BlockSpec(memory_space=pltpu.VMEM)
SMEM = pl.BlockSpec(memory_space=pltpu.SMEM)
ANY = pl.BlockSpec(memory_space=pl.ANY)


def params(mib):
    return pltpu.CompilerParams(vmem_limit_bytes=mib << 20)


def cost(flops, size):
    return pl.CostEstimate(flops=flops, bytes_accessed=size, transcendentals=0)


def per_device(sources, tree_perm, leaf_blocks, u_factors, v_factors, level_ranks):
    row_count, rhs_count = sources.shape
    leaf_size = leaf_blocks.shape[1]
    level_count, rank_cap, _ = u_factors.shape
    dev_bits = (lax.axis_size("row") * lax.axis_size("col")).bit_length() - 1
    half = rank_cap // 2
    coarse = (dev_bits - 1) * half
    total = 2 * coarse + rank_cap
    lanes = 128
    perm = tree_perm.reshape(row_count // lanes, lanes)
    near_rows = sum(rank_cap << level - dev_bits + 1 for level in range(dev_bits, level_count))

    send, keep = pl.pallas_call(
        functools.partial(coef_kernel, dev_bits),
        out_shape=(
            jax.ShapeDtypeStruct((coarse + rank_cap, rhs_count), F32),
            jax.ShapeDtypeStruct((coarse, rhs_count), F32),
        ),
        in_specs=[SMEM, VMEM, VMEM, ANY],
        out_specs=(VMEM, VMEM),
        scratch_shapes=[
            pltpu.VMEM((row_count, row_count), BF16),
            pltpu.VMEM((total, row_count), BF16),
            pltpu.VMEM((row_count, rhs_count), BF16),
            pltpu.SemaphoreType.DMA,
        ],
        compiler_params=params(16),
        cost_estimate=cost(2 * total * row_count * (row_count + rhs_count), 2 << 20),
        name="coef",
    )(level_ranks, perm, v_factors, sources)

    ordered = pl.pallas_call(
        order_kernel,
        out_shape=jax.ShapeDtypeStruct((row_count, rhs_count), BF16),
        in_specs=[VMEM, VMEM],
        out_specs=VMEM,
        scratch_shapes=[pltpu.VMEM((row_count, row_count), BF16)],
        compiler_params=params(16),
        cost_estimate=cost(2 * row_count * row_count * rhs_count, 2 << 20),
        name="order",
    )(perm, sources)

    near, u_far = pl.pallas_call(
        functools.partial(near_kernel, dev_bits),
        out_shape=(
            jax.ShapeDtypeStruct((row_count, rhs_count), F32),
            jax.ShapeDtypeStruct((row_count, total), BF16),
        ),
        in_specs=[SMEM, VMEM, VMEM, VMEM, VMEM, VMEM],
        out_specs=(VMEM, VMEM),
        scratch_shapes=[
            pltpu.VMEM((row_count, row_count), BF16),
            pltpu.VMEM((row_count, row_count + near_rows), BF16),
            pltpu.VMEM((row_count + near_rows, rhs_count), BF16),
        ],
        compiler_params=params(28),
        cost_estimate=cost(2 * row_count * row_count * (leaf_size + rhs_count + total), 6 << 20),
        name="near",
    )(level_ranks, perm, leaf_blocks, u_factors, v_factors, ordered)

    received = partner(send, 0)
    running = keep + received[:coarse]
    sibling = received[coarse:]
    far = []
    for bit in range(1, dev_bits):
        received = partner(running, bit)
        far.insert(0, received[-half:])
        running = running[:-half] + received[:-half]
    mine = jnp.concatenate(far, axis=0)
    other = partner(mine, 0)

    block = row_count // 4
    return pl.pallas_call(
        functools.partial(far_kernel, block),
        out_shape=jax.ShapeDtypeStruct((row_count, rhs_count), BF16),
        in_specs=[VMEM] * 5,
        out_specs=ANY,
        scratch_shapes=[
            pltpu.VMEM((total, rhs_count), BF16),
            pltpu.VMEM((row_count, rhs_count), BF16),
            pltpu.SemaphoreType.DMA((row_count // block,)),
        ],
        compiler_params=params(16),
        cost_estimate=cost(2 * row_count * total * rhs_count, 5 << 20),
        name="far",
    )(near, u_far, mine, other, sibling)


def solution(mesh):
    placed = (
        P(("row", "col"), None),
        P(("row", "col")),
        P(("row", "col"), None),
        P(None, None, ("row", "col")),
        P(None, None, ("row", "col")),
        P(),
    )
    return jax.shard_map(
        per_device, mesh=mesh, in_specs=placed, out_specs=P(("row", "col"), None), check_vma=False
    )
```

```python
import functools

import jax
import jax.numpy as jnp
from jax import lax
from jax.experimental import pallas as pl
from jax.experimental.pallas import tpu as pltpu
from jax.sharding import PartitionSpec as P


AXES = ("row", "col")
BF16, F32 = jnp.bfloat16, jnp.float32


def partner(x, bit):
    count = lax.axis_size("row") * lax.axis_size("col")
    return lax.ppermute(x, AXES, [(i, i ^ 1 << bit) for i in range(count)])


def local_positions(perm_ref, row_count):
    return lax.rem(perm_ref[...], row_count)


def fill_select(select_ref, index):
    blocks, width = index.shape
    columns = index.T
    lane = lax.broadcasted_iota(jnp.int32, (width, blocks * width), 1)
    for block in range(blocks):
        hit = lane == columns[:, block : block + 1]
        select_ref[block * width : (block + 1) * width, :] = jnp.where(hit, 1.0, 0.0).astype(BF16)


def fill_select_t(select_ref, index):
    blocks, width = index.shape
    sublane = lax.broadcasted_iota(jnp.int32, (blocks * width, width), 0)
    for block in range(blocks):
        hit = sublane == index[block : block + 1, :]
        select_ref[:, block * width : (block + 1) * width] = jnp.where(hit, 1.0, 0.0).astype(BF16)


def dot(a, b):
    return jnp.dot(a, b, preferred_element_type=F32)


def dot_t(a, b):
    return lax.dot_general(a, b, (((1,), (1,)), ((), ())), preferred_element_type=F32)


def coef_kernel(dev_bits, ranks_hbm, perm_hbm, v_hbm, sources_hbm, send_ref, keep_ref,
                select, sources, v, perm, ranks, v_rows, sems):
    copies = [
        pltpu.make_async_copy(source, target, sems.at[at])
        for at, (source, target) in enumerate(
            ((perm_hbm, perm), (ranks_hbm, ranks), (v_hbm, v), (sources_hbm, sources))
        )
    ]
    for copy in copies:
        copy.start()
    rank_cap, row_count = v.shape[1:]
    half = rank_cap // 2
    coarse = (dev_bits - 1) * half
    core = lax.rem(lax.axis_index("col"), 2)
    iota = lax.broadcasted_iota(jnp.int32, (half, 1), 0)

    def masked(level, start):
        rows = v[level, pl.ds(pl.multiple_of(start, half), half), :]
        return jnp.where(iota + start < ranks[level], rows.astype(F32), 0.0).astype(BF16)

    copies[0].wait()
    fill_select(select, local_positions(perm, row_count))
    copies[1].wait()
    copies[2].wait()
    for level in range(dev_bits - 1):
        v_rows[level * half : (level + 1) * half, :] = masked(level, (1 - core) * half)
        at = coarse + rank_cap + level * half
        v_rows[at : at + half, :] = masked(level, core * half)
    for part in range(2):
        at = coarse + part * half
        v_rows[at : at + half, :] = masked(dev_bits - 1, jnp.int32(part * half))
    v_local = dot(v_rows[...], select[...]).astype(BF16)
    copies[3].wait()
    coef = dot(v_local, sources[...])
    send_ref[...] = coef[: coarse + rank_cap]
    keep_ref[...] = coef[coarse + rank_cap :]


def order_kernel(dev_bits, ranks_ref, perm_ref, sources_ref, v_ref, ordered_ref, near_far_ref, select):
    level_count, rank_cap, row_count = v_ref.shape
    fill_select(select, local_positions(perm_ref, row_count))
    ordered_ref[...] = dot(select[...], sources_ref[...]).astype(BF16)
    iota = lax.broadcasted_iota(jnp.int32, (rank_cap, 1), 0)
    row = 0
    for level in range(dev_bits, level_count):
        cluster = row_count >> level - dev_bits + 1
        keep = iota < ranks_ref[level]
        for group in range(row_count // cluster):
            at = slice(group * cluster, (group + 1) * cluster)
            coef = dot(v_ref[level, :, at], ordered_ref[at, :])
            other = row + (group ^ 1) * rank_cap
            near_far_ref[other : other + rank_cap, :] = jnp.where(keep, coef, 0.0).astype(BF16)
        row += row_count // cluster * rank_cap


def leaf_kernel(dev_bits, perm_ref, leaf_ref, u_ref, left_ref, u_far_ref, select_t):
    level_count, rank_cap, row_count = u_ref.shape
    half = rank_cap // 2
    coarse = (dev_bits - 1) * half
    leaf_size = leaf_ref.shape[1]
    core = lax.rem(lax.axis_index("col"), 2)
    fill_select_t(select_t, local_positions(perm_ref, row_count))
    for leaf in range(row_count // leaf_size):
        at = slice(leaf * leaf_size, (leaf + 1) * leaf_size)
        left_ref[:, at] = dot(select_t[:, at], leaf_ref[at, :]).astype(BF16)
    rows = []
    for start in (core * half, (1 - core) * half):
        for level in range(dev_bits - 1):
            rows.append(u_ref[level, pl.ds(pl.multiple_of(start, half), half), :])
    rows.append(u_ref[dev_bits - 1])
    column = 2 * coarse + rank_cap
    u_far_ref[:, :column] = dot_t(select_t[...], jnp.concatenate(rows, axis=0)).astype(BF16)
    for level in range(dev_bits, level_count):
        cluster = row_count >> level - dev_bits + 1
        for group in range(row_count // cluster):
            at = slice(group * cluster, (group + 1) * cluster)
            part = dot_t(select_t[:, at], u_ref[level, :, at])
            u_far_ref[:, column : column + rank_cap] = part.astype(BF16)
            column += rank_cap


def near_kernel(left_ref, ordered_ref, near_ref):
    near_ref[...] = dot(left_ref[...], ordered_ref[...])


def far_kernel(block, near_ref, u_far_ref, mine_ref, other_ref, first_ref, near_far_ref, out_ref, far, out, sems):
    coarse = mine_ref.shape[0]
    rank_cap = first_ref.shape[0] - coarse
    far[:coarse, :] = mine_ref[...].astype(BF16)
    far[coarse : 2 * coarse, :] = other_ref[...].astype(BF16)
    far[2 * coarse : 2 * coarse + rank_cap, :] = first_ref[coarse:, :].astype(BF16)
    far[2 * coarse + rank_cap :, :] = near_far_ref[...]
    copies = []
    for step in range(near_ref.shape[0] // block):
        at = slice(step * block, (step + 1) * block)
        out[at, :] = (near_ref[at, :] + dot(u_far_ref[at, :], far[...])).astype(BF16)
        copy = pltpu.make_async_copy(out.at[at, :], out_ref.at[at, :], sems.at[step])
        copy.start()
        copies.append(copy)
    for copy in copies:
        copy.wait()


VMEM = pl.BlockSpec(memory_space=pltpu.VMEM)
SMEM = pl.BlockSpec(memory_space=pltpu.SMEM)
HBM = pl.BlockSpec(memory_space=pltpu.HBM)


def params(mib):
    return pltpu.CompilerParams(vmem_limit_bytes=mib << 20)


def cost(flops, size):
    return pl.CostEstimate(flops=flops, bytes_accessed=size, transcendentals=0)


def like(shape, dtype):
    return jax.ShapeDtypeStruct(shape, dtype)


def exchange(send, keep, half, dev_bits):
    count = 1 << dev_bits
    coarse = keep.shape[0]
    first = lax.rem(lax.axis_index("col"), 2) == 1

    def crossed(x, bits):
        return lax.ppermute(x, AXES, [(i, i ^ 1 << bits[i & 1]) for i in range(count)])

    received = partner(send, 0)
    running = keep + received[:coarse]
    first_received = received
    received = crossed(running, (2, 1))
    met = received[-2 * half : -half]
    summed = running[:-half] + received[:-half]
    one = received[-half:]
    again = jnp.where(first, summed[-half:], met)
    running = jnp.concatenate([summed[:-half], again, running[-half:]], axis=0)
    received = crossed(running, (1, 2))
    far = [
        received[-2 * half : -half] + jnp.where(first, 0.0, met),
        jnp.where(first, one, received[-half:]),
    ]
    running = running[: -2 * half] + received[: -2 * half]
    for bit in range(3, dev_bits):
        received = partner(running, bit)
        far.insert(0, received[-half:])
        running = running[:-half] + received[:-half]
    mine = jnp.concatenate(far, axis=0)
    return mine, partner(mine, 0), first_received


def per_device(sources, tree_perm, leaf_blocks, u_factors, v_factors, level_ranks):
    row_count, rhs_count = sources.shape
    leaf_size = leaf_blocks.shape[1]
    level_count, rank_cap, _ = u_factors.shape
    dev_bits = (lax.axis_size("row") * lax.axis_size("col")).bit_length() - 1
    half = rank_cap // 2
    coarse = (dev_bits - 1) * half
    total = 2 * coarse + rank_cap
    lanes = 128
    perm_shape = (row_count // lanes, lanes)
    near_rows = sum(rank_cap << level - dev_bits + 1 for level in range(dev_bits, level_count))

    def in_hbm(x):
        return pltpu.with_memory_space_constraint(x, pltpu.HBM)

    perm = tree_perm.reshape(perm_shape)
    send, keep = pl.pallas_call(
        functools.partial(coef_kernel, dev_bits),
        out_shape=(like((coarse + rank_cap, rhs_count), F32), like((coarse, rhs_count), F32)),
        in_specs=[HBM] * 4,
        out_specs=(VMEM,) * 2,
        scratch_shapes=[
            pltpu.VMEM((row_count, row_count), BF16),
            pltpu.VMEM(sources.shape, BF16),
            pltpu.VMEM(v_factors.shape, BF16),
            pltpu.VMEM(perm_shape, jnp.int32),
            pltpu.SMEM((level_count,), jnp.int32),
            pltpu.VMEM((total, row_count), BF16),
            pltpu.SemaphoreType.DMA((4,)),
        ],
        compiler_params=params(16),
        cost_estimate=cost(2 * total * row_count * (row_count + rhs_count), 2 << 20),
        name="coef",
    )(in_hbm(level_ranks), in_hbm(perm), in_hbm(v_factors), in_hbm(sources))

    ordered, near_far = pl.pallas_call(
        functools.partial(order_kernel, dev_bits),
        out_shape=(like(sources.shape, BF16), like((near_rows, rhs_count), BF16)),
        in_specs=[SMEM] + [VMEM] * 3,
        out_specs=(VMEM,) * 2,
        scratch_shapes=[pltpu.VMEM((row_count, row_count), BF16)],
        compiler_params=params(16),
        cost_estimate=cost(2 * row_count * row_count * rhs_count, 2 << 20),
        name="order",
    )(level_ranks, perm, sources, v_factors)

    left, u_far = pl.pallas_call(
        functools.partial(leaf_kernel, dev_bits),
        out_shape=(like((row_count, row_count), BF16), like((row_count, total + near_rows), BF16)),
        in_specs=[VMEM] * 3,
        out_specs=(VMEM,) * 2,
        scratch_shapes=[pltpu.VMEM((row_count, row_count), BF16)],
        compiler_params=params(16),
        cost_estimate=cost(2 * row_count * row_count * (leaf_size + total), 4 << 20),
        name="leaf",
    )(perm, leaf_blocks, u_factors)

    near = pl.pallas_call(
        near_kernel,
        out_shape=like((row_count, rhs_count), F32),
        in_specs=[VMEM] * 2,
        out_specs=VMEM,
        compiler_params=params(16),
        cost_estimate=cost(2 * row_count * row_count * rhs_count, 6 << 20),
        name="near",
    )(left, ordered)

    mine, other, received = exchange(send, keep, half, dev_bits)

    block = row_count // 4
    return pl.pallas_call(
        functools.partial(far_kernel, block),
        out_shape=like((row_count, rhs_count), BF16),
        in_specs=[VMEM] * 6,
        out_specs=HBM,
        scratch_shapes=[
            pltpu.VMEM((total + near_rows, rhs_count), BF16),
            pltpu.VMEM((row_count, rhs_count), BF16),
            pltpu.SemaphoreType.DMA((row_count // block,)),
        ],
        compiler_params=params(16),
        cost_estimate=cost(2 * row_count * total * rhs_count, 5 << 20),
        name="far",
    )(near, u_far, mine, other, received, near_far)


def solution(mesh):
    placed = (
        P(("row", "col"), None),
        P(("row", "col")),
        P(("row", "col"), None),
        P(None, None, ("row", "col")),
        P(None, None, ("row", "col")),
        P(),
    )

    return jax.shard_map(
        per_device, mesh=mesh, in_specs=placed, out_specs=P(("row", "col"), None), check_vma=False
    )
```

```python
import functools

import jax
import jax.numpy as jnp
from jax import lax
from jax.experimental import pallas as pl
from jax.experimental.pallas import tpu as pltpu
from jax.sharding import PartitionSpec as P


AXES = ("row", "col")
BF16, F32 = jnp.bfloat16, jnp.float32


def parity(index, bits):
    folded = index
    for bit in range(1, bits):
        folded = folded ^ index >> bit
    return folded & 1


def half_index(dev_bits):
    return parity(lax.axis_index("row") * lax.axis_size("col") + lax.axis_index("col"), dev_bits)


def core_swap(x, dev_bits):
    return lax.ppermute(x, AXES, [(i, i ^ 1) for i in range(1 << dev_bits)])


def chip_swap(x, dev_bits, bits):
    pairs = [(i, i ^ 1 << bits[parity(i, dev_bits)] ^ 1) for i in range(1 << dev_bits)]
    return lax.ppermute(x, AXES, pairs)


def local_positions(perm_ref, row_count):
    return lax.rem(perm_ref[...], row_count)


def fill_select(select_ref, index):
    blocks, width = index.shape
    columns = index.T
    lane = lax.broadcasted_iota(jnp.int32, (width, blocks * width), 1)
    for block in range(blocks):
        hit = lane == columns[:, block : block + 1]
        select_ref[block * width : (block + 1) * width, :] = jnp.where(hit, 1.0, 0.0).astype(BF16)


def fill_select_t(select_ref, index):
    blocks, width = index.shape
    sublane = lax.broadcasted_iota(jnp.int32, (blocks * width, width), 0)
    for block in range(blocks):
        hit = sublane == index[block : block + 1, :]
        select_ref[:, block * width : (block + 1) * width] = jnp.where(hit, 1.0, 0.0).astype(BF16)


def dot(a, b):
    return jnp.dot(a, b, preferred_element_type=F32)


def dot_t(a, b):
    return lax.dot_general(a, b, (((1,), (1,)), ((), ())), preferred_element_type=F32)


def coef_kernel(dev_bits, ranks_hbm, perm_hbm, v_hbm, sources_hbm, u_hbm,
                send_ref, keep_ref, near_far_ref, perm, u,
                select, sources, v, ranks, v_rows, sems):
    copies = [
        pltpu.make_async_copy(source, target, sems.at[at])
        for at, (source, target) in enumerate(
            ((perm_hbm, perm), (ranks_hbm, ranks), (v_hbm, v), (sources_hbm, sources), (u_hbm, u))
        )
    ]
    for copy in copies:
        copy.start()
    level_count, rank_cap, row_count = v.shape
    half = rank_cap // 2
    coarse = (dev_bits - 1) * half
    core = half_index(dev_bits)
    iota = lax.broadcasted_iota(jnp.int32, (half, 1), 0)

    def masked(level, start):
        rows = v[level, pl.ds(pl.multiple_of(start, half), half), :]
        return jnp.where(iota + start < ranks[level], rows.astype(F32), 0.0).astype(BF16)

    copies[0].wait()
    fill_select(select, local_positions(perm, row_count))
    copies[1].wait()
    copies[2].wait()
    for level in range(dev_bits - 1):
        v_rows[level * half : (level + 1) * half, :] = masked(level, (1 - core) * half)
        at = coarse + rank_cap + level * half
        v_rows[at : at + half, :] = masked(level, core * half)
    for part in range(2):
        at = coarse + part * half
        v_rows[at : at + half, :] = masked(dev_bits - 1, jnp.int32(part * half))
    row = 2 * coarse + rank_cap
    column = lax.broadcasted_iota(jnp.int32, (1, row_count), 1)
    rank = lax.broadcasted_iota(jnp.int32, (rank_cap, 1), 0)
    for level in range(dev_bits, level_count):
        cluster = row_count >> level - dev_bits + 1
        groups = row_count // cluster
        rows = jnp.where(rank < ranks[level], v[level].astype(F32), 0.0)
        for group in range(groups):
            other = group ^ 1
            inside = (column >= other * cluster) & (column < (other + 1) * cluster)
            v_rows[row : row + rank_cap, :] = jnp.where(inside, rows, 0.0).astype(BF16)
            row += rank_cap
    v_local = dot(v_rows[...], select[...]).astype(BF16)
    copies[3].wait()
    coef = dot(v_local, sources[...])
    split = coarse + rank_cap
    send_ref[...] = coef[:split]
    keep_ref[...] = coef[split : split + coarse]
    near_far_ref[...] = coef[split + coarse :].astype(BF16)
    copies[4].wait()


def basis_kernel(dev_bits, perm_ref, u_ref, select_t, u_far_ref):
    level_count, rank_cap, row_count = u_ref.shape
    half = rank_cap // 2
    coarse = (dev_bits - 1) * half
    core = half_index(dev_bits)
    fill_select_t(select_t, local_positions(perm_ref, row_count))
    rows = []
    for start in (core * half, (1 - core) * half):
        for level in range(dev_bits - 1):
            rows.append(u_ref[level, pl.ds(pl.multiple_of(start, half), half), :])
    rows.append(u_ref[dev_bits - 1])
    column = 2 * coarse + rank_cap
    u_far_ref[:, :column] = dot_t(select_t[...], jnp.concatenate(rows, axis=0)).astype(BF16)
    for level in range(dev_bits, level_count):
        cluster = row_count >> level - dev_bits + 1
        for group in range(row_count // cluster):
            at = slice(group * cluster, (group + 1) * cluster)
            part = dot_t(select_t[:, at], u_ref[level, :, at])
            u_far_ref[:, column : column + rank_cap] = part.astype(BF16)
            column += rank_cap


def leaf_kernel(perm_ref, select_t, leaf_ref, left_ref, select):
    row_count, leaf_size = leaf_ref.shape
    for leaf in range(row_count // leaf_size):
        at = slice(leaf * leaf_size, (leaf + 1) * leaf_size)
        left_ref[:, at] = dot(select_t[:, at], leaf_ref[at, :]).astype(BF16)
    fill_select(select, local_positions(perm_ref, row_count))


def order_kernel(select_ref, sources_ref, ordered_ref):
    ordered_ref[...] = dot(select_ref[...], sources_ref[...]).astype(BF16)


def near_kernel(left_ref, ordered_ref, near_ref):
    near_ref[...] = dot(left_ref[...], ordered_ref[...])


def far_kernel(block, near_ref, u_far_ref, mine_ref, other_ref, first_ref, near_far_ref, out_ref, far, out, sems):
    coarse = mine_ref.shape[0]
    rank_cap = first_ref.shape[0] - coarse
    far[:coarse, :] = mine_ref[...].astype(BF16)
    far[coarse : 2 * coarse, :] = other_ref[...].astype(BF16)
    far[2 * coarse : 2 * coarse + rank_cap, :] = first_ref[coarse:, :].astype(BF16)
    far[2 * coarse + rank_cap :, :] = near_far_ref[...]
    copies = []
    for step in range(near_ref.shape[0] // block):
        at = slice(step * block, (step + 1) * block)
        out[at, :] = (near_ref[at, :] + dot(u_far_ref[at, :], far[...])).astype(BF16)
        copy = pltpu.make_async_copy(out.at[at, :], out_ref.at[at, :], sems.at[step])
        copy.start()
        copies.append(copy)
    for copy in copies:
        copy.wait()


VMEM = pl.BlockSpec(memory_space=pltpu.VMEM)
SMEM = pl.BlockSpec(memory_space=pltpu.SMEM)
HBM = pl.BlockSpec(memory_space=pltpu.HBM)


def params(mib):
    return pltpu.CompilerParams(vmem_limit_bytes=mib << 20)


def cost(flops, size):
    return pl.CostEstimate(flops=flops, bytes_accessed=size, transcendentals=0)


def like(shape, dtype):
    return jax.ShapeDtypeStruct(shape, dtype)


def exchange(send, keep, half, dev_bits):
    top = dev_bits - 1
    coarse = keep.shape[0]
    second = half_index(dev_bits) == 1

    first = core_swap(send, dev_bits)
    running = keep + first[:coarse]

    def add_unless(drop, own, received):
        if drop == (False, False):
            return own + received
        if drop == (True, True):
            return received
        return received + jnp.where(second if drop[1] else jnp.logical_not(second), 0.0, own)

    def settle(own, arrived, step):
        if step == 1:
            met.append(arrived[-half:])
            last = add_unless((True, False), own[-2 * half : -half], arrived[-2 * half : -half])
            return jnp.concatenate([own[: -2 * half] + arrived[: -2 * half], last, own[-half:]], axis=0)
        if step == 2:
            far[top - 1] = jnp.where(second, met[0], arrived[-half:])
            far[top - 2] = add_unless((False, True), own[-2 * half : -half], arrived[-2 * half : -half])
            return own[: -2 * half] + arrived[: -2 * half]
        far[top - step] = arrived[-half:]
        return own[:-half] + arrived[:-half]

    met = []
    head, rest = running[:half], running[half:]
    far = [None] * top
    straight = list(range(3, top - 1))
    head_bits = list(zip([2, 1] + straight + [top, top - 1], [1, 2] + straight + [top - 1, top]))
    rest_bits = [(2, 1), (1, 2)] + [(bit, bit) for bit in range(3, top)]
    arriving = None
    for step in range(top):
        bits = head_bits[step]
        received = chip_swap(head, dev_bits, bits)
        if arriving is not None:
            rest = settle(rest, arriving, step)
        if step < top - 1:
            arriving = chip_swap(rest, dev_bits, rest_bits[step])
        head = add_unless((bits[0] == top, bits[1] == top), head, received)
        if step < top - 1:
            _, arriving = lax.optimization_barrier((head, arriving))
    far[0] = head
    mine = jnp.concatenate(far, axis=0)
    return mine, core_swap(mine, dev_bits), first


def per_device(sources, tree_perm, leaf_blocks, u_factors, v_factors, level_ranks):
    row_count, rhs_count = sources.shape
    leaf_size = leaf_blocks.shape[1]
    level_count, rank_cap, _ = u_factors.shape
    dev_bits = (lax.axis_size("row") * lax.axis_size("col")).bit_length() - 1
    half = rank_cap // 2
    coarse = (dev_bits - 1) * half
    total = 2 * coarse + rank_cap
    lanes = 128
    perm_shape = (row_count // lanes, lanes)
    near_rows = sum(rank_cap << level - dev_bits + 1 for level in range(dev_bits, level_count))

    def in_hbm(x):
        return pltpu.with_memory_space_constraint(x, pltpu.HBM)

    send, keep, near_far, perm, u_in = pl.pallas_call(
        functools.partial(coef_kernel, dev_bits),
        out_shape=(
            like((coarse + rank_cap, rhs_count), F32),
            like((coarse, rhs_count), F32),
            like((near_rows, rhs_count), BF16),
            like(perm_shape, jnp.int32),
            like(u_factors.shape, BF16),
        ),
        in_specs=[HBM] * 5,
        out_specs=(VMEM,) * 5,
        scratch_shapes=[
            pltpu.VMEM((row_count, row_count), BF16),
            pltpu.VMEM(sources.shape, BF16),
            pltpu.VMEM(v_factors.shape, BF16),
            pltpu.SMEM((level_count,), jnp.int32),
            pltpu.VMEM((total + near_rows, row_count), BF16),
            pltpu.SemaphoreType.DMA((5,)),
        ],
        compiler_params=params(16),
        cost_estimate=cost(2 * total * row_count * (row_count + rhs_count), 2 << 20),
        name="coef",
    )(*map(in_hbm, (level_ranks, tree_perm.reshape(perm_shape), v_factors, sources, u_factors)))

    select_t, u_far = pl.pallas_call(
        functools.partial(basis_kernel, dev_bits),
        out_shape=(like((row_count, row_count), BF16), like((row_count, total + near_rows), BF16)),
        in_specs=[VMEM] * 2,
        out_specs=(VMEM,) * 2,
        compiler_params=params(16),
        cost_estimate=cost(2 * row_count * row_count * total, 3 << 20),
        name="basis",
    )(perm, u_in)

    left, select = pl.pallas_call(
        leaf_kernel,
        out_shape=(like((row_count, row_count), BF16),) * 2,
        in_specs=[VMEM] * 3,
        out_specs=(VMEM,) * 2,
        compiler_params=params(16),
        cost_estimate=cost(2 * row_count * row_count * leaf_size, 4 << 20),
        name="leaf",
    )(perm, select_t, leaf_blocks)

    ordered = pl.pallas_call(
        order_kernel,
        out_shape=like(sources.shape, BF16),
        in_specs=[VMEM] * 2,
        out_specs=VMEM,
        compiler_params=params(16),
        cost_estimate=cost(2 * row_count * row_count * rhs_count, 2 << 20),
        name="order",
    )(select, sources)

    near = pl.pallas_call(
        near_kernel,
        out_shape=like((row_count, rhs_count), F32),
        in_specs=[VMEM] * 2,
        out_specs=VMEM,
        compiler_params=params(16),
        cost_estimate=cost(2 * row_count * row_count * rhs_count, 6 << 20),
        name="near",
    )(left, ordered)

    mine, other, received = exchange(send, keep, half, dev_bits)

    block = row_count // 4
    return pl.pallas_call(
        functools.partial(far_kernel, block),
        out_shape=like((row_count, rhs_count), BF16),
        in_specs=[VMEM] * 6,
        out_specs=HBM,
        scratch_shapes=[
            pltpu.VMEM((total + near_rows, rhs_count), BF16),
            pltpu.VMEM((row_count, rhs_count), BF16),
            pltpu.SemaphoreType.DMA((row_count // block,)),
        ],
        compiler_params=params(16),
        cost_estimate=cost(2 * row_count * total * rhs_count, 5 << 20),
        name="far",
    )(near, u_far, mine, other, received, near_far)


def solution(mesh):
    placed = (
        P(("row", "col"), None),
        P(("row", "col")),
        P(("row", "col"), None),
        P(None, None, ("row", "col")),
        P(None, None, ("row", "col")),
        P(),
    )

    return jax.shard_map(
        per_device, mesh=mesh, in_specs=placed, out_specs=P(("row", "col"), None), check_vma=False
    )
```

```python
import functools

import jax
import jax.numpy as jnp
from jax import lax
from jax.experimental import pallas as pl
from jax.experimental.pallas import tpu as pltpu
from jax.sharding import PartitionSpec as P


AXES = ("row", "col")
BF16, F32 = jnp.bfloat16, jnp.float32


def parity(index, bits):
    folded = index
    for bit in range(1, bits):
        folded = folded ^ index >> bit
    return folded & 1


def half_index(dev_bits):
    return parity(lax.axis_index("row") * lax.axis_size("col") + lax.axis_index("col"), dev_bits)


def core_swap(x, dev_bits):
    return lax.ppermute(x, AXES, [(i, i ^ 1) for i in range(1 << dev_bits)])


def chip_swap(x, dev_bits, bits):
    pairs = [(i, i ^ 1 << bits[parity(i, dev_bits)] ^ 1) for i in range(1 << dev_bits)]
    return lax.ppermute(x, AXES, pairs)


def local_positions(perm_ref, row_count, start=0, stop=None):
    blocks, width = perm_ref.shape
    stop = blocks * width if stop is None else stop
    return lax.rem(perm_ref[start // width : stop // width, :], row_count)


def fill_select(select_ref, index, row_count):
    blocks, width = index.shape
    columns = index.T
    lane = lax.broadcasted_iota(jnp.int32, (width, row_count), 1)
    for block in range(blocks):
        hit = lane == columns[:, block : block + 1]
        select_ref[block * width : (block + 1) * width, :] = jnp.where(hit, 1.0, 0.0).astype(BF16)


def fill_select_t(select_ref, index, row_count):
    blocks, width = index.shape
    sublane = lax.broadcasted_iota(jnp.int32, (row_count, width), 0)
    for block in range(blocks):
        hit = sublane == index[block : block + 1, :]
        select_ref[:, block * width : (block + 1) * width] = jnp.where(hit, 1.0, 0.0).astype(BF16)


def cluster_columns(row_count, depth):
    cluster = row_count >> depth
    column = lax.broadcasted_iota(jnp.int32, (1, row_count), 1)
    return [
        (column >= start) & (column < start + cluster) for start in range(0, row_count, cluster)
    ]


def dot(a, b):
    return jnp.dot(a, b, preferred_element_type=F32)


def dot_t(a, b):
    return lax.dot_general(a, b, (((1,), (1,)), ((), ())), preferred_element_type=F32)


def coef_kernel(dev_bits, ranks_hbm, perm_hbm, v_hbm, sources_hbm, u_hbm,
                send_ref, keep_ref, near_far_ref, perm, u,
                select, sources, v, ranks, v_rows, sems):
    copies = [
        pltpu.make_async_copy(source, target, sems.at[at])
        for at, (source, target) in enumerate(
            ((perm_hbm, perm), (ranks_hbm, ranks), (v_hbm, v), (sources_hbm, sources), (u_hbm, u))
        )
    ]
    for copy in copies:
        copy.start()
    level_count, rank_cap, row_count = v.shape
    half = rank_cap // 2
    coarse = (dev_bits - 1) * half
    core = half_index(dev_bits)
    iota = lax.broadcasted_iota(jnp.int32, (half, 1), 0)

    def masked(level, start):
        rows = v[level, pl.ds(pl.multiple_of(start, half), half), :]
        return jnp.where(iota + start < ranks[level], rows.astype(F32), 0.0).astype(BF16)

    copies[0].wait()
    fill_select(select, local_positions(perm, row_count), row_count)
    copies[1].wait()
    copies[2].wait()
    for level in range(dev_bits - 1):
        v_rows[level * half : (level + 1) * half, :] = masked(level, (1 - core) * half)
        at = coarse + rank_cap + level * half
        v_rows[at : at + half, :] = masked(level, core * half)
    for part in range(2):
        at = coarse + part * half
        v_rows[at : at + half, :] = masked(dev_bits - 1, jnp.int32(part * half))
    row = 2 * coarse + rank_cap
    rank = lax.broadcasted_iota(jnp.int32, (rank_cap, 1), 0)
    for level in range(dev_bits, level_count):
        rows = jnp.where(rank < ranks[level], v[level].astype(F32), 0.0)
        clusters = cluster_columns(row_count, level - dev_bits + 1)
        for group in range(len(clusters)):
            v_rows[row : row + rank_cap, :] = jnp.where(clusters[group ^ 1], rows, 0.0).astype(BF16)
            row += rank_cap
    v_local = dot(v_rows[...], select[...]).astype(BF16)
    copies[3].wait()
    coef = dot(v_local, sources[...])
    split = coarse + rank_cap
    send_ref[...] = coef[:split]
    keep_ref[...] = coef[split : split + coarse]
    near_far_ref[...] = coef[split + coarse :].astype(BF16)
    copies[4].wait()


def basis_kernel(dev_bits, perm_ref, u_ref, u_far_ref, select_t):
    level_count, rank_cap, row_count = u_ref.shape
    half = rank_cap // 2
    core = half_index(dev_bits)
    fill_select_t(select_t, local_positions(perm_ref, row_count), row_count)
    rows = []
    for start in (core * half, (1 - core) * half):
        for level in range(dev_bits - 1):
            rows.append(u_ref[level, pl.ds(pl.multiple_of(start, half), half), :])
    rows.append(u_ref[dev_bits - 1])
    for level in range(dev_bits, level_count):
        for inside in cluster_columns(row_count, level - dev_bits + 1):
            rows.append(jnp.where(inside, u_ref[level].astype(F32), 0.0).astype(BF16))
    u_far_ref[...] = dot_t(select_t[...], jnp.concatenate(rows, axis=0)).astype(BF16)


def order_kernel(start, stop, perm_ref, sources_ref, ordered_ref, select):
    row_count = sources_ref.shape[0]
    fill_select(select, local_positions(perm_ref, row_count, start, stop), row_count)
    ordered_ref[...] = dot(select[...], sources_ref[...]).astype(BF16)


def leaf_kernel(leaf, perm_ref, block_ref, left_ref, select_t):
    row_count, leaf_size = block_ref.shape
    start, stop = leaf * leaf_size, (leaf + 1) * leaf_size
    fill_select_t(select_t, local_positions(perm_ref, row_count, start, stop), row_count)
    left_ref[...] = dot(select_t[...], block_ref[start:stop, :]).astype(BF16)


def near_kernel(leaves, pieces, *refs):
    lefts, ordered, near_ref = refs[:leaves], refs[leaves:-1], refs[-1]
    leaf_size = lefts[0].shape[1]
    parts = []
    for (start, stop), piece in zip(pieces, ordered):
        at = slice(start % leaf_size, start % leaf_size + stop - start)
        parts.append(dot(lefts[start // leaf_size][:, at], piece[...]))
    near_ref[...] = sum(parts)


def far_kernel(block, near_ref, u_far_ref, mine_ref, other_ref, first_ref, near_far_ref, out_ref, far, out, sems):
    coarse = mine_ref.shape[0]
    rank_cap = first_ref.shape[0] - coarse
    far[:coarse, :] = mine_ref[...].astype(BF16)
    far[coarse : 2 * coarse, :] = other_ref[...].astype(BF16)
    far[2 * coarse : 2 * coarse + rank_cap, :] = first_ref[coarse:, :].astype(BF16)
    far[2 * coarse + rank_cap :, :] = near_far_ref[...]
    copies = []
    for step in range(near_ref.shape[0] // block):
        at = slice(step * block, (step + 1) * block)
        out[at, :] = (near_ref[at, :] + dot(u_far_ref[at, :], far[...])).astype(BF16)
        copy = pltpu.make_async_copy(out.at[at, :], out_ref.at[at, :], sems.at[step])
        copy.start()
        copies.append(copy)
    for copy in copies:
        copy.wait()


VMEM = pl.BlockSpec(memory_space=pltpu.VMEM)
SMEM = pl.BlockSpec(memory_space=pltpu.SMEM)
HBM = pl.BlockSpec(memory_space=pltpu.HBM)


def params(mib):
    return pltpu.CompilerParams(vmem_limit_bytes=mib << 20)


def cost(flops, size):
    return pl.CostEstimate(flops=flops, bytes_accessed=size, transcendentals=0)


def like(shape, dtype):
    return jax.ShapeDtypeStruct(shape, dtype)


def exchange(send, keep, half, dev_bits):
    top = dev_bits - 1
    coarse = keep.shape[0]
    second = half_index(dev_bits) == 1

    first = core_swap(send, dev_bits)
    running = keep + first[:coarse]

    def add_unless(drop, own, received):
        if drop == (False, False):
            return own + received
        if drop == (True, True):
            return received
        return received + jnp.where(second if drop[1] else jnp.logical_not(second), 0.0, own)

    def settle(own, arrived, step):
        if step == 1:
            met.append(arrived[-half:])
            last = add_unless((True, False), own[-2 * half : -half], arrived[-2 * half : -half])
            return jnp.concatenate([own[: -2 * half] + arrived[: -2 * half], last, own[-half:]], axis=0)
        if step == 2:
            far[top - 1] = jnp.where(second, met[0], arrived[-half:])
            far[top - 2] = add_unless((False, True), own[-2 * half : -half], arrived[-2 * half : -half])
            return own[: -2 * half] + arrived[: -2 * half]
        far[top - step] = arrived[-half:]
        return own[:-half] + arrived[:-half]

    met = []
    head, rest = running[:half], running[half:]
    far = [None] * top
    straight = list(range(3, top - 1))
    head_bits = list(zip([2, 1] + straight + [top, top - 1], [1, 2] + straight + [top - 1, top]))
    rest_bits = [(2, 1), (1, 2)] + [(bit, bit) for bit in range(3, top)]
    arriving = None
    for step in range(top):
        bits = head_bits[step]
        received = chip_swap(head, dev_bits, bits)
        if arriving is not None:
            rest = settle(rest, arriving, step)
        if step < top - 1:
            arriving = chip_swap(rest, dev_bits, rest_bits[step])
        head = add_unless((bits[0] == top, bits[1] == top), head, received)
        if step < top - 1:
            _, arriving = lax.optimization_barrier((head, arriving))
    far[0] = head
    mine = jnp.concatenate(far, axis=0)
    return mine, core_swap(mine, dev_bits), first


def per_device(sources, tree_perm, leaf_blocks, u_factors, v_factors, level_ranks):
    row_count, rhs_count = sources.shape
    leaf_size = leaf_blocks.shape[1]
    level_count, rank_cap, _ = u_factors.shape
    dev_bits = (lax.axis_size("row") * lax.axis_size("col")).bit_length() - 1
    half = rank_cap // 2
    coarse = (dev_bits - 1) * half
    total = 2 * coarse + rank_cap
    lanes = 128
    perm_shape = (row_count // lanes, lanes)
    near_rows = sum(rank_cap << level - dev_bits + 1 for level in range(dev_bits, level_count))

    def in_hbm(x):
        return pltpu.with_memory_space_constraint(x, pltpu.HBM)

    send, keep, near_far, perm, u_in = pl.pallas_call(
        functools.partial(coef_kernel, dev_bits),
        out_shape=(
            like((coarse + rank_cap, rhs_count), F32),
            like((coarse, rhs_count), F32),
            like((near_rows, rhs_count), BF16),
            like(perm_shape, jnp.int32),
            like(u_factors.shape, BF16),
        ),
        in_specs=[HBM] * 5,
        out_specs=(VMEM,) * 5,
        scratch_shapes=[
            pltpu.VMEM((row_count, row_count), BF16),
            pltpu.VMEM(sources.shape, BF16),
            pltpu.VMEM(v_factors.shape, BF16),
            pltpu.SMEM((level_count,), jnp.int32),
            pltpu.VMEM((total + near_rows, row_count), BF16),
            pltpu.SemaphoreType.DMA((5,)),
        ],
        compiler_params=params(16),
        cost_estimate=cost(2 * total * row_count * (row_count + rhs_count), 2 << 20),
        name="coef",
    )(*map(in_hbm, (level_ranks, tree_perm.reshape(perm_shape), v_factors, sources, u_factors)))

    u_far = pl.pallas_call(
        functools.partial(basis_kernel, dev_bits),
        out_shape=like((row_count, total + near_rows), BF16),
        in_specs=[VMEM] * 2,
        out_specs=VMEM,
        scratch_shapes=[pltpu.VMEM((row_count, row_count), BF16)],
        compiler_params=params(16),
        cost_estimate=cost(2 * row_count * row_count * total, 3 << 20),
        name="basis",
    )(perm, u_in)

    leaves = row_count // leaf_size
    middle = row_count // 2
    pieces = [(0, middle), (middle, middle + middle // 2), (middle + middle // 2, row_count)]
    ordered, left = [], []
    for start, stop in pieces:
        ordered.append(
            pl.pallas_call(
                functools.partial(order_kernel, start, stop),
                out_shape=like((stop - start, rhs_count), BF16),
                in_specs=[VMEM] * 2,
                out_specs=VMEM,
                scratch_shapes=[pltpu.VMEM((stop - start, row_count), BF16)],
                compiler_params=params(16),
                cost_estimate=cost(2 * (stop - start) * row_count * rhs_count, 2 << 20),
                name="order",
            )(perm, sources)
        )
    for leaf in range(leaves):
        left.append(
            pl.pallas_call(
                functools.partial(leaf_kernel, leaf),
                out_shape=like((row_count, leaf_size), BF16),
                in_specs=[VMEM] * 2,
                out_specs=VMEM,
                scratch_shapes=[pltpu.VMEM((row_count, leaf_size), BF16)],
                compiler_params=params(16),
                cost_estimate=cost(2 * row_count * leaf_size * leaf_size, 2 << 20),
                name="leaf",
            )(perm, leaf_blocks)
        )

    near = pl.pallas_call(
        functools.partial(near_kernel, leaves, pieces),
        out_shape=like((row_count, rhs_count), F32),
        in_specs=[VMEM] * (leaves + len(pieces)),
        out_specs=VMEM,
        compiler_params=params(16),
        cost_estimate=cost(2 * row_count * row_count * rhs_count, 6 << 20),
        name="near",
    )(*left, *ordered)

    mine, other, received = exchange(send, keep, half, dev_bits)

    block = row_count // 8
    return pl.pallas_call(
        functools.partial(far_kernel, block),
        out_shape=like((row_count, rhs_count), BF16),
        in_specs=[VMEM] * 6,
        out_specs=HBM,
        scratch_shapes=[
            pltpu.VMEM((total + near_rows, rhs_count), BF16),
            pltpu.VMEM((row_count, rhs_count), BF16),
            pltpu.SemaphoreType.DMA((row_count // block,)),
        ],
        compiler_params=params(16),
        cost_estimate=cost(2 * row_count * total * rhs_count, 5 << 20),
        name="far",
    )(near, u_far, mine, other, received, near_far)


def solution(mesh):
    placed = (
        P(("row", "col"), None),
        P(("row", "col")),
        P(("row", "col"), None),
        P(None, None, ("row", "col")),
        P(None, None, ("row", "col")),
        P(),
    )

    return jax.shard_map(
        per_device, mesh=mesh, in_specs=placed, out_specs=P(("row", "col"), None), check_vma=False
    )
```

```python
import functools

import jax
import jax.numpy as jnp
from jax import lax
from jax.experimental import pallas as pl
from jax.experimental.pallas import tpu as pltpu
from jax.sharding import PartitionSpec as P


AXES = ("row", "col")
BF16, F32 = jnp.bfloat16, jnp.float32


def parity(index, bits):
    folded = index
    for bit in range(1, bits):
        folded = folded ^ index >> bit
    return folded & 1


def half_index(dev_bits):
    return parity(lax.axis_index("row") * lax.axis_size("col") + lax.axis_index("col"), dev_bits)


def core_swap(x, dev_bits):
    return lax.ppermute(x, AXES, [(i, i ^ 1) for i in range(1 << dev_bits)])


def chip_swap(x, dev_bits, bits):
    pairs = [(i, i ^ 1 << bits[parity(i, dev_bits)] ^ 1) for i in range(1 << dev_bits)]
    return lax.ppermute(x, AXES, pairs)


def local_positions(perm_ref, row_count, start=0, stop=None):
    blocks, width = perm_ref.shape
    stop = blocks * width if stop is None else stop
    return lax.rem(perm_ref[start // width : stop // width, :], row_count)


def fill_select(select_ref, index, row_count):
    blocks, width = index.shape
    columns = index.T.astype(jnp.int16)
    lane = lax.broadcasted_iota(jnp.int32, (width, row_count), 1).astype(jnp.int16)
    for block in range(blocks):
        hit = lane == columns[:, block : block + 1]
        select_ref[block * width : (block + 1) * width, :] = jnp.where(hit, BF16(1), BF16(0))


def fill_select_t(select_ref, index, row_count):
    blocks, width = index.shape
    index = index.astype(jnp.int16)
    sublane = lax.broadcasted_iota(jnp.int32, (row_count, width), 0).astype(jnp.int16)
    for block in range(blocks):
        hit = sublane == jnp.broadcast_to(index[block : block + 1, :], (row_count, width))
        select_ref[:, block * width : (block + 1) * width] = jnp.where(hit, BF16(1), BF16(0))


def cluster_columns(row_count, depth):
    cluster = row_count >> depth
    column = lax.broadcasted_iota(jnp.int32, (1, row_count), 1)
    return [
        jnp.where((column >= start) & (column < start + cluster), 1.0, 0.0).astype(BF16)
        for start in range(0, row_count, cluster)
    ]


def dot(a, b):
    return jnp.dot(a, b, preferred_element_type=F32)


def dot_t(a, b):
    return lax.dot_general(a, b, (((1,), (1,)), ((), ())), preferred_element_type=F32)


def coef_kernel(dev_bits, ranks_hbm, perm_hbm, v_hbm, sources_hbm, u_hbm,
                send_ref, keep_ref, near_0_ref, near_1_ref, perm, u,
                select, sources, v, ranks, v_rows, sems):
    copies = [
        pltpu.make_async_copy(source, target, sems.at[at])
        for at, (source, target) in enumerate(
            ((perm_hbm, perm), (ranks_hbm, ranks), (v_hbm, v), (sources_hbm, sources), (u_hbm, u))
        )
    ]
    for copy in copies:
        copy.start()
    level_count, rank_cap, row_count = v.shape
    half = rank_cap // 2
    coarse = (dev_bits - 1) * half
    core = half_index(dev_bits)
    iota = lax.broadcasted_iota(jnp.int32, (half, 1), 0)

    def masked(level, start):
        rows = v[level, pl.ds(pl.multiple_of(start, half), half), :]
        return rows * jnp.where(iota + start < ranks[level], 1.0, 0.0).astype(BF16)

    copies[0].wait()
    fill_select(select, local_positions(perm, row_count), row_count)
    copies[1].wait()
    copies[2].wait()
    for level in range(dev_bits - 1):
        v_rows[level * half : (level + 1) * half, :] = masked(level, (1 - core) * half)
        at = coarse + rank_cap + level * half
        v_rows[at : at + half, :] = masked(level, core * half)
    for part in range(2):
        at = coarse + part * half
        v_rows[at : at + half, :] = masked(dev_bits - 1, jnp.int32(part * half))
    row = 2 * coarse + rank_cap
    rank = lax.broadcasted_iota(jnp.int32, (rank_cap, 1), 0)
    for level in range(dev_bits, level_count):
        rows = v[level] * jnp.where(rank < ranks[level], 1.0, 0.0).astype(BF16)
        clusters = cluster_columns(row_count, level - dev_bits + 1)
        for group in range(len(clusters)):
            v_rows[row : row + rank_cap, :] = rows * clusters[group ^ 1]
            row += rank_cap
    v_local = dot(v_rows[...], select[...]).astype(BF16)
    copies[3].wait()
    coef = dot(v_local, sources[...])
    split = coarse + rank_cap
    send_ref[...] = coef[:split]
    keep_ref[...] = coef[split : split + coarse]
    near_half = split + coarse + (coef.shape[0] - split - coarse) // 2
    near_0_ref[...] = coef[split + coarse : near_half]
    near_1_ref[...] = coef[near_half:]
    copies[4].wait()


def basis_kernel(dev_bits, perm_ref, u_ref, u_far_ref, select_t):
    level_count, rank_cap, row_count = u_ref.shape
    half = rank_cap // 2
    core = half_index(dev_bits)
    fill_select_t(select_t, local_positions(perm_ref, row_count), row_count)
    rows = []
    for start in (core * half, (1 - core) * half):
        for level in range(dev_bits - 1):
            rows.append(u_ref[level, pl.ds(pl.multiple_of(start, half), half), :])
    rows.append(u_ref[dev_bits - 1])
    for level in range(dev_bits, level_count):
        for inside in cluster_columns(row_count, level - dev_bits + 1):
            rows.append(u_ref[level] * inside)
    u_far_ref[...] = dot_t(select_t[...], jnp.concatenate(rows, axis=0)).astype(BF16)


def order_kernel(start, stop, perm_ref, sources_ref, ordered_ref, select):
    row_count = sources_ref.shape[0]
    fill_select(select, local_positions(perm_ref, row_count, start, stop), row_count)
    ordered_ref[...] = dot(select[...], sources_ref[...]).astype(BF16)


def leaf_kernel(leaf, perm_ref, block_ref, left_ref, select_t):
    row_count, leaf_size = block_ref.shape
    start, stop = leaf * leaf_size, (leaf + 1) * leaf_size
    fill_select_t(select_t, local_positions(perm_ref, row_count, start, stop), row_count)
    left_ref[...] = dot(select_t[...], block_ref[start:stop, :]).astype(BF16)


def near_kernel(leaves, pieces, *refs):
    lefts, ordered, near_ref = refs[:leaves], refs[leaves:-1], refs[-1]
    leaf_size = lefts[0].shape[1]
    parts = []
    for leaf in range(leaves):
        first, last = leaf * leaf_size, (leaf + 1) * leaf_size
        for (start, stop), piece in zip(pieces, ordered):
            low, high = max(start, first), min(stop, last)
            if low < high:
                columns = slice(low - first, high - first)
                parts.append(dot(lefts[leaf][:, columns], piece[low - start : high - start, :]))
    near_ref[...] = sum(parts)


def round_kernel(coef_ref, rounded_ref):
    rounded_ref[...] = coef_ref[...].astype(BF16)


def far_kernel(block, near_ref, u_far_ref, mine_ref, other_ref, first_ref, near_0_ref, near_1_ref,
               out_ref, far, out, sems):
    coarse = mine_ref.shape[0]
    rank_cap = first_ref.shape[0] - coarse
    far[:coarse, :] = mine_ref[...].astype(BF16)
    far[coarse : 2 * coarse, :] = other_ref[...].astype(BF16)
    far[2 * coarse : 2 * coarse + rank_cap, :] = first_ref[coarse:, :].astype(BF16)
    near_half = 2 * coarse + rank_cap + near_0_ref.shape[0]
    far[2 * coarse + rank_cap : near_half, :] = near_0_ref[...]
    far[near_half:, :] = near_1_ref[...]
    copies = []
    for step in range(near_ref.shape[0] // block):
        at = slice(step * block, (step + 1) * block)
        out[at, :] = (near_ref[at, :] + dot(u_far_ref[at, :], far[...])).astype(BF16)
        copy = pltpu.make_async_copy(out.at[at, :], out_ref.at[at, :], sems.at[step])
        copy.start()
        copies.append(copy)
    for copy in copies:
        copy.wait()


VMEM = pl.BlockSpec(memory_space=pltpu.VMEM)
SMEM = pl.BlockSpec(memory_space=pltpu.SMEM)
HBM = pl.BlockSpec(memory_space=pltpu.HBM)


def params(mib):
    return pltpu.CompilerParams(vmem_limit_bytes=mib << 20)


def cost(flops, size):
    return pl.CostEstimate(flops=flops, bytes_accessed=size, transcendentals=0)


def like(shape, dtype):
    return jax.ShapeDtypeStruct(shape, dtype)


def exchange(send, keep, half, dev_bits):
    top = dev_bits - 1
    coarse = keep.shape[0]
    second = half_index(dev_bits) == 1

    first = core_swap(send, dev_bits)
    running = keep + first[:coarse]

    def add_unless(drop, own, received):
        if drop == (False, False):
            return own + received
        if drop == (True, True):
            return received
        return received + jnp.where(second if drop[1] else jnp.logical_not(second), 0.0, own)

    def settle(own, arrived, step):
        if step == 1:
            met.append(arrived[-half:])
            last = add_unless((True, False), own[-2 * half : -half], arrived[-2 * half : -half])
            return jnp.concatenate([own[: -2 * half] + arrived[: -2 * half], last, own[-half:]], axis=0)
        if step == 2:
            far[top - 1] = jnp.where(second, met[0], arrived[-half:])
            far[top - 2] = add_unless((False, True), own[-2 * half : -half], arrived[-2 * half : -half])
            return own[: -2 * half] + arrived[: -2 * half]
        far[top - step] = arrived[-half:]
        return own[:-half] + arrived[:-half]

    met = []
    head, rest = running[:half], running[half:]
    far = [None] * top
    straight = list(range(3, top - 1))
    head_bits = list(zip([2, 1] + straight + [top, top - 1], [1, 2] + straight + [top - 1, top]))
    rest_bits = [(2, 1), (1, 2)] + [(bit, bit) for bit in range(3, top)]
    arriving = None
    for step in range(top):
        bits = head_bits[step]
        received = chip_swap(head, dev_bits, bits)
        if arriving is not None:
            rest = settle(rest, arriving, step)
        if step < top - 1:
            arriving = chip_swap(rest, dev_bits, rest_bits[step])
        head = add_unless((bits[0] == top, bits[1] == top), head, received)
        if step < top - 1:
            _, arriving = lax.optimization_barrier((head, arriving))
    far[0] = head
    mine = jnp.concatenate(far, axis=0)
    return mine, core_swap(mine, dev_bits), first


def per_device(sources, tree_perm, leaf_blocks, u_factors, v_factors, level_ranks):
    row_count, rhs_count = sources.shape
    leaf_size = leaf_blocks.shape[1]
    level_count, rank_cap, _ = u_factors.shape
    dev_bits = (lax.axis_size("row") * lax.axis_size("col")).bit_length() - 1
    half = rank_cap // 2
    coarse = (dev_bits - 1) * half
    total = 2 * coarse + rank_cap
    lanes = 128
    perm_shape = (row_count // lanes, lanes)
    near_rows = sum(rank_cap << level - dev_bits + 1 for level in range(dev_bits, level_count))

    def in_hbm(x):
        return pltpu.with_memory_space_constraint(x, pltpu.HBM)

    send, keep, *near_coef, perm, u_in = pl.pallas_call(
        functools.partial(coef_kernel, dev_bits),
        out_shape=(
            like((coarse + rank_cap, rhs_count), F32),
            like((coarse, rhs_count), F32),
            like((near_rows // 2, rhs_count), F32),
            like((near_rows // 2, rhs_count), F32),
            like(perm_shape, jnp.int32),
            like(u_factors.shape, BF16),
        ),
        in_specs=[HBM] * 5,
        out_specs=(VMEM,) * 6,
        scratch_shapes=[
            pltpu.VMEM((row_count, row_count), BF16),
            pltpu.VMEM(sources.shape, BF16),
            pltpu.VMEM(v_factors.shape, BF16),
            pltpu.SMEM((level_count,), jnp.int32),
            pltpu.VMEM((total + near_rows, row_count), BF16),
            pltpu.SemaphoreType.DMA((5,)),
        ],
        compiler_params=params(16),
        cost_estimate=cost(2 * total * row_count * (row_count + rhs_count), 2 << 20),
        name="coef",
    )(*map(in_hbm, (level_ranks, tree_perm.reshape(perm_shape), v_factors, sources, u_factors)))

    u_far = pl.pallas_call(
        functools.partial(basis_kernel, dev_bits),
        out_shape=like((row_count, total + near_rows), BF16),
        in_specs=[VMEM] * 2,
        out_specs=VMEM,
        scratch_shapes=[pltpu.VMEM((row_count, row_count), BF16)],
        compiler_params=params(16),
        cost_estimate=cost(2 * row_count * row_count * total, 3 << 20),
        name="basis",
    )(perm, u_in)

    leaves = row_count // leaf_size
    cut = row_count * 3 // 4
    pieces = [(0, cut), (cut, row_count)]
    ordered, left = [], []
    for start, stop in pieces:
        ordered.append(
            pl.pallas_call(
                functools.partial(order_kernel, start, stop),
                out_shape=like((stop - start, rhs_count), BF16),
                in_specs=[VMEM] * 2,
                out_specs=VMEM,
                scratch_shapes=[pltpu.VMEM((stop - start, row_count), BF16)],
                compiler_params=params(16),
                cost_estimate=cost(2 * (stop - start) * row_count * rhs_count, 2 << 20),
                name="order",
            )(perm, sources)
        )
    for leaf in range(leaves):
        left.append(
            pl.pallas_call(
                functools.partial(leaf_kernel, leaf),
                out_shape=like((row_count, leaf_size), BF16),
                in_specs=[VMEM] * 2,
                out_specs=VMEM,
                scratch_shapes=[pltpu.VMEM((row_count, leaf_size), BF16)],
                compiler_params=params(16),
                cost_estimate=cost(2 * row_count * leaf_size * leaf_size, 2 << 20),
                name="leaf",
            )(perm, leaf_blocks)
        )

    near = pl.pallas_call(
        functools.partial(near_kernel, leaves, pieces),
        out_shape=like((row_count, rhs_count), F32),
        in_specs=[VMEM] * (leaves + len(pieces)),
        out_specs=VMEM,
        compiler_params=params(16),
        cost_estimate=cost(2 * row_count * row_count * rhs_count, 6 << 20),
        name="near",
    )(*left, *ordered)

    rounded = []
    for rows in near_coef:
        rounded.append(
            pl.pallas_call(
                round_kernel,
                out_shape=like(rows.shape, BF16),
                in_specs=[VMEM],
                out_specs=VMEM,
                compiler_params=params(16),
                cost_estimate=cost(rows.size, 6 * rows.size),
                name="round",
            )(rows)
        )

    mine, other, received = exchange(send, keep, half, dev_bits)

    block = row_count // 8
    return pl.pallas_call(
        functools.partial(far_kernel, block),
        out_shape=like((row_count, rhs_count), BF16),
        in_specs=[VMEM] * 7,
        out_specs=HBM,
        scratch_shapes=[
            pltpu.VMEM((total + near_rows, rhs_count), BF16),
            pltpu.VMEM((row_count, rhs_count), BF16),
            pltpu.SemaphoreType.DMA((row_count // block,)),
        ],
        compiler_params=params(16),
        cost_estimate=cost(2 * row_count * total * rhs_count, 5 << 20),
        name="far",
    )(near, u_far, mine, other, received, *rounded)


def solution(mesh):
    placed = (
        P(("row", "col"), None),
        P(("row", "col")),
        P(("row", "col"), None),
        P(None, None, ("row", "col")),
        P(None, None, ("row", "col")),
        P(),
    )

    return jax.shard_map(
        per_device, mesh=mesh, in_specs=placed, out_specs=P(("row", "col"), None), check_vma=False
    )
```

```python
import functools

import jax
import jax.numpy as jnp
from jax import lax
from jax.experimental import pallas as pl
from jax.experimental.pallas import tpu as pltpu
from jax.sharding import PartitionSpec as P


AXES = ("row", "col")
BF16, F32 = jnp.bfloat16, jnp.float32


def parity(index, bits):
    folded = index
    for bit in range(1, bits):
        folded = folded ^ index >> bit
    return folded & 1


def half_index(dev_bits):
    return parity(lax.axis_index("row") * lax.axis_size("col") + lax.axis_index("col"), dev_bits)


def core_swap(x, dev_bits):
    return lax.ppermute(x, AXES, [(i, i ^ 1) for i in range(1 << dev_bits)])


def chip_swap(x, dev_bits, bits):
    pairs = [(i, i ^ 1 << bits[parity(i, dev_bits)] ^ 1) for i in range(1 << dev_bits)]
    return lax.ppermute(x, AXES, pairs)


def local_positions(perm_ref, row_count, start=0, stop=None):
    blocks, width = perm_ref.shape
    stop = blocks * width if stop is None else stop
    return lax.rem(perm_ref[start // width : stop // width, :], row_count)


def fill_select(select_ref, index, row_count):
    blocks, width = index.shape
    columns = index.T.astype(jnp.int16)
    lane = lax.broadcasted_iota(jnp.int32, (width, row_count), 1).astype(jnp.int16)
    for block in range(blocks):
        hit = lane == columns[:, block : block + 1]
        select_ref[block * width : (block + 1) * width, :] = jnp.where(hit, BF16(1), BF16(0))


def fill_select_t(select_ref, index, row_count):
    blocks, width = index.shape
    index = index.astype(jnp.int16)
    sublane = lax.broadcasted_iota(jnp.int32, (row_count, width), 0).astype(jnp.int16)
    for block in range(blocks):
        hit = sublane == jnp.broadcast_to(index[block : block + 1, :], (row_count, width))
        select_ref[:, block * width : (block + 1) * width] = jnp.where(hit, BF16(1), BF16(0))


def cluster_columns(row_count, depth):
    cluster = row_count >> depth
    column = lax.broadcasted_iota(jnp.int32, (1, row_count), 1)
    return [
        jnp.where((column >= start) & (column < start + cluster), 1.0, 0.0).astype(BF16)
        for start in range(0, row_count, cluster)
    ]


def dot(a, b):
    return jnp.dot(a, b, preferred_element_type=F32)


def dot_t(a, b):
    return lax.dot_general(a, b, (((1,), (1,)), ((), ())), preferred_element_type=F32)


def coef_kernel(dev_bits, ranks_hbm, perm_hbm, v_hbm, sources_hbm, u_hbm,
                send_ref, keep_ref, v_close_ref, perm, u,
                select, sources, v, ranks, v_rows, sems):
    copies = [
        pltpu.make_async_copy(source, target, sems.at[at])
        for at, (source, target) in enumerate(
            ((perm_hbm, perm), (ranks_hbm, ranks), (v_hbm, v), (sources_hbm, sources), (u_hbm, u))
        )
    ]
    for copy in copies:
        copy.start()
    level_count, rank_cap, row_count = v.shape
    half = rank_cap // 2
    coarse = (dev_bits - 1) * half
    core = half_index(dev_bits)
    iota = lax.broadcasted_iota(jnp.int32, (half, 1), 0)

    def masked(level, start):
        rows = v[level, pl.ds(start if isinstance(start, int) else pl.multiple_of(start, half), half), :]
        return rows * jnp.where(iota + start < ranks[level], 1.0, 0.0).astype(BF16)

    copies[0].wait()
    fill_select(select, local_positions(perm, row_count), row_count)
    copies[1].wait()
    copies[2].wait()
    for level in range(dev_bits - 1):
        v_rows[level * half : (level + 1) * half, :] = masked(level, (1 - core) * half)
        at = coarse + rank_cap + level * half
        v_rows[at : at + half, :] = masked(level, core * half)
    for part in range(2):
        at = coarse + part * half
        v_rows[at : at + half, :] = masked(dev_bits - 1, jnp.int32(part * half))
    v_local = dot(v_rows[...], select[...]).astype(BF16)
    for level in range(dev_bits, level_count):
        for part in range(2):
            rows = slice(part * half, (part + 1) * half)
            v_close_ref[level - dev_bits, rows, :] = masked(level, part * half)
    copies[3].wait()
    coef = dot(v_local, sources[...])
    send_ref[...] = coef[: coarse + rank_cap]
    keep_ref[...] = coef[coarse + rank_cap :]
    copies[4].wait()


def basis_kernel(dev_bits, perm_ref, u_ref, u_far_ref, select_t):
    level_count, rank_cap, row_count = u_ref.shape
    half = rank_cap // 2
    core = half_index(dev_bits)
    fill_select_t(select_t, local_positions(perm_ref, row_count), row_count)
    rows = []
    for start in (core * half, (1 - core) * half):
        for level in range(dev_bits - 1):
            rows.append(u_ref[level, pl.ds(pl.multiple_of(start, half), half), :])
    rows.append(u_ref[dev_bits - 1])
    for level in range(dev_bits, level_count):
        for inside in cluster_columns(row_count, level - dev_bits + 1):
            rows.append(u_ref[level] * inside)
    u_far_ref[...] = dot_t(select_t[...], jnp.concatenate(rows, axis=0)).astype(BF16)


def order_kernel(start, stop, perm_ref, sources_ref, ordered_ref, select):
    row_count = sources_ref.shape[0]
    fill_select(select, local_positions(perm_ref, row_count, start, stop), row_count)
    ordered_ref[...] = dot(select[...], sources_ref[...]).astype(BF16)


def leaf_kernel(leaf, perm_ref, block_ref, v_close_ref, left_ref, select_t):
    row_count, leaf_size = block_ref.shape
    close_count, rank_cap, _ = v_close_ref.shape
    at = slice(leaf * leaf_size, (leaf + 1) * leaf_size)
    fill_select_t(select_t, local_positions(perm_ref, row_count, at.start, at.stop), row_count)
    left_ref[:row_count, :] = dot(select_t[...], block_ref[at, :]).astype(BF16)
    row = row_count
    for level in range(close_count):
        kept = v_close_ref[level, :, at]
        cluster = row_count >> level + 1
        for group in range(row_count // cluster):
            other = group ^ 1
            low = max(other * cluster, at.start) - at.start
            high = min((other + 1) * cluster, at.stop) - at.start
            if high - low < leaf_size:
                left_ref[row : row + rank_cap, :] = jnp.zeros((rank_cap, leaf_size), BF16)
            if low < high:
                left_ref[row : row + rank_cap, low:high] = kept[:, low:high]
            row += rank_cap


def near_kernel(leaf, pieces, *refs):
    left_ref, ordered, near_ref = refs[0], refs[1 : 1 + len(pieces)], refs[-1]
    leaf_size = left_ref.shape[1]
    first, last = leaf * leaf_size, (leaf + 1) * leaf_size
    parts = [refs[-2][...]] if len(refs) == len(pieces) + 3 else []
    for (start, stop), piece in zip(pieces, ordered):
        low, high = max(start, first), min(stop, last)
        parts.append(dot(left_ref[:, low - first : high - first], piece[low - start : high - start, :]))
    near_ref[...] = sum(parts)


def round_kernel(start, coef_ref, rounded_ref):
    rounded_ref[...] = coef_ref[start : start + rounded_ref.shape[0], :].astype(BF16)


def far_kernel(block, near_ref, u_far_ref, mine_ref, other_ref, sibling_0_ref, sibling_1_ref,
               out_ref, far, out, sems):
    row = 0
    row_count = out.shape[0]
    for part in (mine_ref, other_ref, sibling_0_ref, sibling_1_ref, near_ref.at[row_count:, :]):
        far[row : row + part.shape[0], :] = part[...].astype(BF16)
        row += part.shape[0]
    copies = []
    for step in range(row_count // block):
        at = slice(step * block, (step + 1) * block)
        out[at, :] = (near_ref[at, :] + dot(u_far_ref[at, :], far[...])).astype(BF16)
        copy = pltpu.make_async_copy(out.at[at, :], out_ref.at[at, :], sems.at[step])
        copy.start()
        copies.append(copy)
    for copy in copies:
        copy.wait()


VMEM = pl.BlockSpec(memory_space=pltpu.VMEM)
SMEM = pl.BlockSpec(memory_space=pltpu.SMEM)
HBM = pl.BlockSpec(memory_space=pltpu.HBM)


def params(mib):
    return pltpu.CompilerParams(vmem_limit_bytes=mib << 20)


def cost(flops, size):
    return pl.CostEstimate(flops=flops, bytes_accessed=size, transcendentals=0)


def like(shape, dtype):
    return jax.ShapeDtypeStruct(shape, dtype)


def exchange(send, keep, half, dev_bits):
    top = dev_bits - 1
    coarse = keep.shape[0]
    second = half_index(dev_bits) == 1

    first = core_swap(send, dev_bits)
    running = keep + first[:coarse]

    def add_unless(drop, own, received):
        if drop == (False, False):
            return own + received
        if drop == (True, True):
            return received
        return received + jnp.where(second if drop[1] else jnp.logical_not(second), 0.0, own)

    def settle(own, arrived, step):
        if step == 1:
            met.append(arrived[-half:])
            last = add_unless((True, False), own[-2 * half : -half], arrived[-2 * half : -half])
            return jnp.concatenate([own[: -2 * half] + arrived[: -2 * half], last, own[-half:]], axis=0)
        if step == 2:
            far[top - 1] = jnp.where(second, met[0], arrived[-half:])
            far[top - 2] = add_unless((False, True), own[-2 * half : -half], arrived[-2 * half : -half])
            return own[: -2 * half] + arrived[: -2 * half]
        far[top - step] = arrived[-half:]
        return own[:-half] + arrived[:-half]

    met = []
    head, rest = running[:half], running[half:]
    far = [None] * top
    straight = list(range(3, top - 1))
    head_bits = list(zip([2, 1] + straight + [top, top - 1], [1, 2] + straight + [top, top - 1]))
    rest_bits = [(2, 1), (1, 2)] + [(bit, bit) for bit in range(3, top)]
    arriving = None
    for step in range(top):
        bits = head_bits[step]
        received = chip_swap(head, dev_bits, bits)
        if arriving is not None:
            rest = settle(rest, arriving, step)
        if step < top - 1:
            arriving = chip_swap(rest, dev_bits, rest_bits[step])
        head = add_unless((bits[0] == top, bits[1] == top), head, received)
        if step < top - 1:
            _, arriving = lax.optimization_barrier((head, arriving))
    far[0] = head
    mine = jnp.concatenate(far, axis=0)
    return mine, core_swap(mine, dev_bits), first


def per_device(sources, tree_perm, leaf_blocks, u_factors, v_factors, level_ranks):
    row_count, rhs_count = sources.shape
    leaf_size = leaf_blocks.shape[1]
    level_count, rank_cap, _ = u_factors.shape
    dev_bits = (lax.axis_size("row") * lax.axis_size("col")).bit_length() - 1
    half = rank_cap // 2
    coarse = (dev_bits - 1) * half
    total = 2 * coarse + rank_cap
    lanes = 128
    perm_shape = (row_count // lanes, lanes)
    near_rows = sum(rank_cap << level - dev_bits + 1 for level in range(dev_bits, level_count))

    def in_hbm(x):
        return pltpu.with_memory_space_constraint(x, pltpu.HBM)

    send, keep, v_close, perm, u_in = pl.pallas_call(
        functools.partial(coef_kernel, dev_bits),
        out_shape=(
            like((coarse + rank_cap, rhs_count), F32),
            like((coarse, rhs_count), F32),
            like((level_count - dev_bits, rank_cap, row_count), BF16),
            like(perm_shape, jnp.int32),
            like(u_factors.shape, BF16),
        ),
        in_specs=[HBM] * 5,
        out_specs=(VMEM,) * 5,
        scratch_shapes=[
            pltpu.VMEM((row_count, row_count), BF16),
            pltpu.VMEM(sources.shape, BF16),
            pltpu.VMEM(v_factors.shape, BF16),
            pltpu.SMEM((level_count,), jnp.int32),
            pltpu.VMEM((total, row_count), BF16),
            pltpu.SemaphoreType.DMA((5,)),
        ],
        compiler_params=params(16),
        cost_estimate=cost(2 * total * row_count * (row_count + rhs_count), 2 << 20),
        name="coef",
    )(*map(in_hbm, (level_ranks, tree_perm.reshape(perm_shape), v_factors, sources, u_factors)))

    u_far = pl.pallas_call(
        functools.partial(basis_kernel, dev_bits),
        out_shape=like((row_count, total + near_rows), BF16),
        in_specs=[VMEM] * 2,
        out_specs=VMEM,
        scratch_shapes=[pltpu.VMEM((row_count, row_count), BF16)],
        compiler_params=params(16),
        cost_estimate=cost(2 * row_count * row_count * total, 3 << 20),
        name="basis",
    )(perm, u_in)

    leaves = row_count // leaf_size
    cut = row_count * 3 // 4
    pieces = [(0, cut), (cut, row_count)]
    ordered, left = [], []
    for start, stop in pieces:
        ordered.append(
            pl.pallas_call(
                functools.partial(order_kernel, start, stop),
                out_shape=like((stop - start, rhs_count), BF16),
                in_specs=[VMEM] * 2,
                out_specs=VMEM,
                scratch_shapes=[pltpu.VMEM((stop - start, row_count), BF16)],
                compiler_params=params(16),
                cost_estimate=cost(2 * (stop - start) * row_count * rhs_count, 2 << 20),
                name="order",
            )(perm, sources)
        )
    for leaf in range(leaves):
        left.append(
            pl.pallas_call(
                functools.partial(leaf_kernel, leaf),
                out_shape=like((row_count + near_rows, leaf_size), BF16),
                in_specs=[VMEM] * 3,
                out_specs=VMEM,
                scratch_shapes=[pltpu.VMEM((row_count, leaf_size), BF16)],
                compiler_params=params(16),
                cost_estimate=cost(2 * row_count * leaf_size * leaf_size, 2 << 20),
                name="leaf",
            )(perm, leaf_blocks, v_close)
        )

    near = None
    for leaf in reversed(range(leaves)):
        inside = [
            number
            for number, (start, stop) in enumerate(pieces)
            if start < (leaf + 1) * leaf_size and stop > leaf * leaf_size
        ]
        operands = [left[leaf], *(ordered[number] for number in inside)]
        operands += [] if near is None else [near]
        near = pl.pallas_call(
            functools.partial(near_kernel, leaf, [pieces[number] for number in inside]),
            out_shape=like((row_count + near_rows, rhs_count), F32),
            in_specs=[VMEM] * len(operands),
            out_specs=VMEM,
            input_output_aliases={} if near is None else {len(operands) - 1: 0},
            compiler_params=params(16),
            cost_estimate=cost(2 * row_count * leaf_size * rhs_count, 6 << 20),
            name="near",
        )(*operands)

    mine, other, received = exchange(send, keep, half, dev_bits)

    sibling = []
    for number in range(2):
        sibling.append(
            pl.pallas_call(
                functools.partial(round_kernel, coarse + number * half),
                out_shape=like((half, rhs_count), BF16),
                in_specs=[VMEM],
                out_specs=VMEM,
                compiler_params=params(16),
                cost_estimate=cost(half * rhs_count, 6 * half * rhs_count),
                name="round",
            )(received)
        )

    block = row_count // 8
    return pl.pallas_call(
        functools.partial(far_kernel, block),
        out_shape=like((row_count, rhs_count), BF16),
        in_specs=[VMEM] * 6,
        out_specs=HBM,
        scratch_shapes=[
            pltpu.VMEM((total + near_rows, rhs_count), BF16),
            pltpu.VMEM((row_count, rhs_count), BF16),
            pltpu.SemaphoreType.DMA((row_count // block,)),
        ],
        compiler_params=params(16),
        cost_estimate=cost(2 * row_count * total * rhs_count, 5 << 20),
        name="far",
    )(near, u_far, mine, other, *sibling)


def solution(mesh):
    placed = (
        P(("row", "col"), None),
        P(("row", "col")),
        P(("row", "col"), None),
        P(None, None, ("row", "col")),
        P(None, None, ("row", "col")),
        P(),
    )

    return jax.shard_map(
        per_device, mesh=mesh, in_specs=placed, out_specs=P(("row", "col"), None), check_vma=False
    )
```

```python
import functools

import jax
import jax.numpy as jnp
from jax import lax
from jax.experimental import pallas as pl
from jax.experimental.pallas import tpu as pltpu
from jax.sharding import PartitionSpec as P


AXES = ("row", "col")
BF16, F32 = jnp.bfloat16, jnp.float32


def parity(index, bits):
    folded = index
    for bit in range(1, bits):
        folded = folded ^ index >> bit
    return folded & 1


def half_index(dev_bits):
    return parity(lax.axis_index("row") * lax.axis_size("col") + lax.axis_index("col"), dev_bits)


def core_swap(x, dev_bits):
    return lax.ppermute(x, AXES, [(i, i ^ 1) for i in range(1 << dev_bits)])


def chip_swap(x, dev_bits, bits):
    pairs = [(i, i ^ 1 << bits[parity(i, dev_bits)] ^ 1) for i in range(1 << dev_bits)]
    return lax.ppermute(x, AXES, pairs)


def local_positions(perm_ref, row_count, start=0, stop=None):
    blocks, width = perm_ref.shape
    stop = blocks * width if stop is None else stop
    return lax.rem(perm_ref[start // width : stop // width, :], row_count)


def fill_select(select_ref, index, row_count):
    blocks, width = index.shape
    columns = index.T.astype(jnp.int16)
    lane = lax.broadcasted_iota(jnp.int32, (width, row_count), 1).astype(jnp.int16)
    for block in range(blocks):
        hit = lane == columns[:, block : block + 1]
        select_ref[block * width : (block + 1) * width, :] = jnp.where(hit, BF16(1), BF16(0))


def fill_select_t(select_ref, index, row_count):
    blocks, width = index.shape
    index = index.astype(jnp.int16)
    sublane = lax.broadcasted_iota(jnp.int32, (row_count, width), 0).astype(jnp.int16)
    for block in range(blocks):
        hit = sublane == jnp.broadcast_to(index[block : block + 1, :], (row_count, width))
        select_ref[:, block * width : (block + 1) * width] = jnp.where(hit, BF16(1), BF16(0))


def cluster_columns(row_count, depth):
    cluster = row_count >> depth
    column = lax.broadcasted_iota(jnp.int32, (1, row_count), 1)
    return [
        jnp.where((column >= start) & (column < start + cluster), 1.0, 0.0).astype(BF16)
        for start in range(0, row_count, cluster)
    ]


def dot(a, b):
    return jnp.dot(a, b, preferred_element_type=F32)


def dot_t(a, b):
    return lax.dot_general(a, b, (((1,), (1,)), ((), ())), preferred_element_type=F32)


def coef_kernel(dev_bits, ranks_hbm, perm_hbm, v_hbm, sources_hbm, u_hbm,
                send_ref, keep_ref, v_close_ref, perm, u,
                select, sources, v, ranks, v_rows, sems):
    copies = [
        pltpu.make_async_copy(source, target, sems.at[at])
        for at, (source, target) in enumerate(
            ((perm_hbm, perm), (ranks_hbm, ranks), (v_hbm, v), (sources_hbm, sources), (u_hbm, u))
        )
    ]
    for copy in copies:
        copy.start()
    level_count, rank_cap, row_count = v.shape
    half = rank_cap // 2
    coarse = (dev_bits - 1) * half
    core = half_index(dev_bits)
    iota = lax.broadcasted_iota(jnp.int32, (half, 1), 0)

    def masked(level, start):
        rows = v[level, pl.ds(start if isinstance(start, int) else pl.multiple_of(start, half), half), :]
        return rows * jnp.where(iota + start < ranks[level], 1.0, 0.0).astype(BF16)

    copies[0].wait()
    fill_select(select, local_positions(perm, row_count), row_count)
    copies[1].wait()
    copies[2].wait()
    for level in range(dev_bits - 1):
        v_rows[level * half : (level + 1) * half, :] = masked(level, (1 - core) * half)
        at = coarse + rank_cap + level * half
        v_rows[at : at + half, :] = masked(level, core * half)
    for part in range(2):
        at = coarse + part * half
        v_rows[at : at + half, :] = masked(dev_bits - 1, jnp.int32(part * half))
    v_local = dot(v_rows[...], select[...]).astype(BF16)
    for level in range(dev_bits, level_count):
        for part in range(2):
            rows = slice(part * half, (part + 1) * half)
            v_close_ref[level - dev_bits, rows, :] = masked(level, part * half)
    copies[3].wait()
    coef = dot(v_local, sources[...])
    send_ref[...] = coef[: coarse + rank_cap]
    keep_ref[...] = coef[coarse + rank_cap :]
    copies[4].wait()


def basis_kernel(dev_bits, perm_ref, u_ref, u_far_ref, select_t):
    level_count, rank_cap, row_count = u_ref.shape
    half = rank_cap // 2
    core = half_index(dev_bits)
    fill_select_t(select_t, local_positions(perm_ref, row_count), row_count)
    rows = []
    for start in (core * half, (1 - core) * half):
        for level in range(dev_bits - 1):
            rows.append(u_ref[level, pl.ds(pl.multiple_of(start, half), half), :])
    rows.append(u_ref[dev_bits - 1])
    for level in range(dev_bits, level_count):
        for inside in cluster_columns(row_count, level - dev_bits + 1):
            rows.append(u_ref[level] * inside)
    u_far_ref[...] = dot_t(select_t[...], jnp.concatenate(rows, axis=0)).astype(BF16)


def order_kernel(start, stop, perm_ref, sources_ref, ordered_ref, select):
    row_count = sources_ref.shape[0]
    fill_select(select, local_positions(perm_ref, row_count, start, stop), row_count)
    ordered_ref[...] = dot(select[...], sources_ref[...]).astype(BF16)


def leaf_kernel(leaf, perm_ref, block_ref, v_close_ref, left_ref, select_t):
    row_count, leaf_size = block_ref.shape
    close_count, rank_cap, _ = v_close_ref.shape
    at = slice(leaf * leaf_size, (leaf + 1) * leaf_size)
    fill_select_t(select_t, local_positions(perm_ref, row_count, at.start, at.stop), row_count)
    left_ref[:row_count, :] = dot(select_t[...], block_ref[at, :]).astype(BF16)
    row = row_count
    for level in range(close_count):
        kept = v_close_ref[level, :, at]
        cluster = row_count >> level + 1
        for group in range(row_count // cluster):
            other = group ^ 1
            low = max(other * cluster, at.start) - at.start
            high = min((other + 1) * cluster, at.stop) - at.start
            if high - low < leaf_size:
                left_ref[row : row + rank_cap, :] = jnp.zeros((rank_cap, leaf_size), BF16)
            if low < high:
                left_ref[row : row + rank_cap, low:high] = kept[:, low:high]
            row += rank_cap


def near_kernel(leaf, pieces, *refs):
    left_ref, ordered, near_ref = refs[0], refs[1 : 1 + len(pieces)], refs[-1]
    leaf_size = left_ref.shape[1]
    first, last = leaf * leaf_size, (leaf + 1) * leaf_size
    parts = [refs[-2][...]] if len(refs) == len(pieces) + 3 else []
    for (start, stop), piece in zip(pieces, ordered):
        low, high = max(start, first), min(stop, last)
        parts.append(dot(left_ref[:, low - first : high - first], piece[low - start : high - start, :]))
    near_ref[...] = sum(parts)


def round_kernel(start, coef_ref, rounded_ref):
    rounded_ref[...] = coef_ref[start : start + rounded_ref.shape[0], :].astype(BF16)


def far_kernel(block, near_ref, u_far_ref, mine_ref, other_ref, sibling_0_ref, sibling_1_ref,
               out_ref, far, out, sems):
    row = 0
    row_count = out.shape[0]
    for part in (mine_ref, other_ref, sibling_0_ref, sibling_1_ref, near_ref.at[row_count:, :]):
        far[row : row + part.shape[0], :] = part[...].astype(BF16)
        row += part.shape[0]
    copies = []
    for step in range(row_count // block):
        at = slice(step * block, (step + 1) * block)
        out[at, :] = (near_ref[at, :] + dot(u_far_ref[at, :], far[...])).astype(BF16)
        copy = pltpu.make_async_copy(out.at[at, :], out_ref.at[at, :], sems.at[step])
        copy.start()
        copies.append(copy)
    for copy in copies:
        copy.wait()


VMEM = pl.BlockSpec(memory_space=pltpu.VMEM)
SMEM = pl.BlockSpec(memory_space=pltpu.SMEM)
HBM = pl.BlockSpec(memory_space=pltpu.HBM)


def params(mib):
    return pltpu.CompilerParams(vmem_limit_bytes=mib << 20)


def cost(flops, size):
    return pl.CostEstimate(flops=flops, bytes_accessed=size, transcendentals=0)


def like(shape, dtype):
    return jax.ShapeDtypeStruct(shape, dtype)


def exchange(send, keep, half, dev_bits):
    top = dev_bits - 1
    coarse = keep.shape[0]
    second = half_index(dev_bits) == 1

    first = core_swap(send, dev_bits)
    running = keep + first[:coarse]

    def add_unless(drop, own, received):
        if drop == (False, False):
            return own + received
        if drop == (True, True):
            return received
        return received + jnp.where(second if drop[1] else jnp.logical_not(second), 0.0, own)

    def settle(own, arrived, step):
        if step == 1:
            met.append(arrived[-half:])
            last = add_unless((True, False), own[-2 * half : -half], arrived[-2 * half : -half])
            return jnp.concatenate([own[: -2 * half] + arrived[: -2 * half], last, own[-half:]], axis=0)
        if step == 2:
            far[top - 1] = jnp.where(second, met[0], arrived[-half:])
            far[top - 2] = add_unless((False, True), own[-2 * half : -half], arrived[-2 * half : -half])
            return own[: -2 * half] + arrived[: -2 * half]
        far[top - step] = arrived[-half:]
        return own[:-half] + arrived[:-half]

    met = []
    head, rest = running[:half], running[half:]
    far = [None] * top
    straight = list(range(3, top - 1))
    head_bits = list(zip([2, 1] + straight + [top, top - 1], [1, 2] + straight + [top, top - 1]))
    rest_bits = [(2, 1), (1, 2)] + [(bit, bit) for bit in range(3, top)]
    arriving = None
    for step in range(top):
        bits = head_bits[step]
        received = chip_swap(head, dev_bits, bits)
        if arriving is not None:
            rest = settle(rest, arriving, step)
        if step < top - 1:
            arriving = chip_swap(rest, dev_bits, rest_bits[step])
        head = add_unless((bits[0] == top, bits[1] == top), head, received)
        if step < top - 1:
            _, arriving = lax.optimization_barrier((head, arriving))
    far[0] = head
    mine = jnp.concatenate(far, axis=0)
    return mine, core_swap(mine, dev_bits), first


def per_device(sources, tree_perm, leaf_blocks, u_factors, v_factors, level_ranks):
    row_count, rhs_count = sources.shape
    leaf_size = leaf_blocks.shape[1]
    level_count, rank_cap, _ = u_factors.shape
    dev_bits = (lax.axis_size("row") * lax.axis_size("col")).bit_length() - 1
    half = rank_cap // 2
    coarse = (dev_bits - 1) * half
    total = 2 * coarse + rank_cap
    lanes = 128
    perm_shape = (row_count // lanes, lanes)
    near_rows = sum(rank_cap << level - dev_bits + 1 for level in range(dev_bits, level_count))

    def in_hbm(x):
        return pltpu.with_memory_space_constraint(x, pltpu.HBM)

    send, keep, v_close, perm, u_in = pl.pallas_call(
        functools.partial(coef_kernel, dev_bits),
        out_shape=(
            like((coarse + rank_cap, rhs_count), F32),
            like((coarse, rhs_count), F32),
            like((level_count - dev_bits, rank_cap, row_count), BF16),
            like(perm_shape, jnp.int32),
            like(u_factors.shape, BF16),
        ),
        in_specs=[HBM] * 5,
        out_specs=(VMEM,) * 5,
        scratch_shapes=[
            pltpu.VMEM((row_count, row_count), BF16),
            pltpu.VMEM(sources.shape, BF16),
            pltpu.VMEM(v_factors.shape, BF16),
            pltpu.SMEM((level_count,), jnp.int32),
            pltpu.VMEM((total, row_count), BF16),
            pltpu.SemaphoreType.DMA((5,)),
        ],
        compiler_params=params(16),
        cost_estimate=cost(2 * total * row_count * (row_count + rhs_count), 2 << 20),
        name="coef",
    )(*map(in_hbm, (level_ranks, tree_perm.reshape(perm_shape), v_factors, sources, u_factors)))

    u_far = pl.pallas_call(
        functools.partial(basis_kernel, dev_bits),
        out_shape=like((row_count, total + near_rows), BF16),
        in_specs=[VMEM] * 2,
        out_specs=VMEM,
        scratch_shapes=[pltpu.VMEM((row_count, row_count), BF16)],
        compiler_params=params(16),
        cost_estimate=cost(2 * row_count * row_count * total, 3 << 20),
        name="basis",
    )(perm, u_in)

    leaves = row_count // leaf_size
    pieces = [(0, row_count)]
    ordered, left = [], []
    for start, stop in pieces:
        ordered.append(
            pl.pallas_call(
                functools.partial(order_kernel, start, stop),
                out_shape=like((stop - start, rhs_count), BF16),
                in_specs=[VMEM] * 2,
                out_specs=VMEM,
                scratch_shapes=[pltpu.VMEM((stop - start, row_count), BF16)],
                compiler_params=params(16),
                cost_estimate=cost(2 * (stop - start) * row_count * rhs_count, 2 << 20),
                name="order",
            )(perm, sources)
        )
    for leaf in range(leaves):
        left.append(
            pl.pallas_call(
                functools.partial(leaf_kernel, leaf),
                out_shape=like((row_count + near_rows, leaf_size), BF16),
                in_specs=[VMEM] * 3,
                out_specs=VMEM,
                scratch_shapes=[pltpu.VMEM((row_count, leaf_size), BF16)],
                compiler_params=params(16),
                cost_estimate=cost(2 * row_count * leaf_size * leaf_size, 2 << 20),
                name="leaf",
            )(perm, leaf_blocks, v_close)
        )

    near = None
    for leaf in reversed(range(leaves)):
        inside = [
            number
            for number, (start, stop) in enumerate(pieces)
            if start < (leaf + 1) * leaf_size and stop > leaf * leaf_size
        ]
        operands = [left[leaf], *(ordered[number] for number in inside)]
        operands += [] if near is None else [near]
        near = pl.pallas_call(
            functools.partial(near_kernel, leaf, [pieces[number] for number in inside]),
            out_shape=like((row_count + near_rows, rhs_count), F32),
            in_specs=[VMEM] * len(operands),
            out_specs=VMEM,
            input_output_aliases={} if near is None else {len(operands) - 1: 0},
            compiler_params=params(16),
            cost_estimate=cost(2 * row_count * leaf_size * rhs_count, 6 << 20),
            name="near",
        )(*operands)

    mine, other, received = exchange(send, keep, half, dev_bits)

    sibling = []
    for number in range(2):
        sibling.append(
            pl.pallas_call(
                functools.partial(round_kernel, coarse + number * half),
                out_shape=like((half, rhs_count), BF16),
                in_specs=[VMEM],
                out_specs=VMEM,
                compiler_params=params(16),
                cost_estimate=cost(half * rhs_count, 6 * half * rhs_count),
                name="round",
            )(received)
        )

    block = row_count // 4
    return pl.pallas_call(
        functools.partial(far_kernel, block),
        out_shape=like((row_count, rhs_count), BF16),
        in_specs=[VMEM] * 6,
        out_specs=HBM,
        scratch_shapes=[
            pltpu.VMEM((total + near_rows, rhs_count), BF16),
            pltpu.VMEM((row_count, rhs_count), BF16),
            pltpu.SemaphoreType.DMA((row_count // block,)),
        ],
        compiler_params=params(16),
        cost_estimate=cost(2 * row_count * total * rhs_count, 5 << 20),
        name="far",
    )(near, u_far, mine, other, *sibling)


def solution(mesh):
    placed = (
        P(("row", "col"), None),
        P(("row", "col")),
        P(("row", "col"), None),
        P(None, None, ("row", "col")),
        P(None, None, ("row", "col")),
        P(),
    )

    return jax.shard_map(
        per_device, mesh=mesh, in_specs=placed, out_specs=P(("row", "col"), None), check_vma=False
    )
```
